128 devices in a mesh: fsdp: 32 (over x, y, core), dp: 4 (over z).
Axes of the slice: x: 4, y: 4, z: 4, core: 2. Of those that a mesh axis runs over, the one named last changes fastest.
Arguments:
- tokens: bfloat16 [65536, 4096], P(('fsdp', 'dp')), may hold values from -40 to 40
- cotangent: bfloat16 [65536, 2048], P(('fsdp', 'dp')), may hold values from -20 to 20
- weight: bfloat16 [4096, 2048], P('fsdp'), may hold values from -1 to 1
- left_vector: float32 [4096], P('fsdp'), may hold values from -6 to 6
Outputs:
- layer_out: bfloat16 [65536, 2048], P(('fsdp', 'dp'))
- input_grad: bfloat16 [65536, 4096], P(('fsdp', 'dp'))
- update: bfloat16 [4096, 2048], P('fsdp')
- left_next: float32 [4096], P('fsdp')
- right_next: float32 [2048], replicated
The draws below stay inside these ranges and needn't reach their ends.
All inputs are finite; a program needn't handle non-finite values.
Results may differ from the reference program's by a relative error of at most 0.015.
Values may be sent and summed in bfloat16 or wider, within the bound.
A program may use at most 128 MiB of HBM per device.

```python
import math
import jax
import jax.numpy as jnp
from jax import lax

D = 4096
TOK_DEV = 512
OUT = 2048
TOKENS = 65536
N_FSDP = 32


token_share = 3.0


cotangent_share = 3.0


spike_gain = 3.0


def base_values(key, rows, columns):
    values = jnp.clip(jax.random.normal(key, (rows, columns), jnp.float32), -6.0, 6.0)
    return values


def common_parts(key):
    weight_key = jax.random.fold_in(key, 11)
    direction_key = jax.random.fold_in(key, 12)
    latent_key = jax.random.fold_in(key, 13)
    weight_raw = base_values(weight_key, D, OUT)
    weight_value = (weight_raw * (1.0 / math.sqrt(D))).astype(jnp.bfloat16).astype(jnp.float32)
    direction = jax.random.normal(direction_key, (D,), jnp.float32)
    direction = direction / jnp.sqrt(jnp.sum(direction * direction))
    latent = jnp.clip(jax.random.normal(latent_key, (TOKENS,), jnp.float32), -4.0, 4.0)
    return (weight_value, direction, latent)


def draw_weight(key, part):
    weight_value, direction, latent = common_parts(key)
    return weight_value.astype(jnp.bfloat16)


def draw_tokens(key, part):
    weight_value, direction, latent = common_parts(key)
    random_key = jax.random.fold_in(key, 21)
    pairing_key = jax.random.fold_in(key, 22)
    values = base_values(random_key, TOKENS, D)
    block_count = TOKENS // TOK_DEV
    pairing = (jax.random.permutation(pairing_key, block_count) % N_FSDP).astype(jnp.int32)
    row_block = (jnp.arange(TOKENS) // TOK_DEV).astype(jnp.int32)
    column_block = (jnp.arange(D) // (D // N_FSDP)).astype(jnp.int32)
    paired = pairing[row_block]
    boost = 1.0 + spike_gain * (paired[:, None] == column_block[None, :]).astype(jnp.float32)
    values = values * boost + token_share * latent[:, None] * direction[None, :]
    return values.astype(jnp.bfloat16)


def draw_cotangent(key, part):
    weight_value, direction, latent = common_parts(key)
    random_key = jax.random.fold_in(key, 31)
    along = jnp.dot(direction, weight_value, precision=lax.Precision.HIGHEST)
    along = along / jnp.sqrt(jnp.sum(along * along))
    values = base_values(random_key, TOKENS, OUT)
    values = values + cotangent_share * latent[:, None] * along[None, :]
    return values.astype(jnp.bfloat16)


def shard_levels(rng, shape, cuts, low, high):
    factor_of, own = 1.0, jax.random.fold_in(rng, 6)
    for axis_at, shards_of in cuts:
        heights = jnp.exp(jax.random.uniform(jax.random.fold_in(own, axis_at), (shards_of,), jnp.float32, low / len(cuts), high / len(cuts)))
        factor_of = factor_of * jnp.repeat(heights, shape[axis_at] // shards_of).reshape([-1 if axis == axis_at else 1 for axis in range(len(shape))])
    return factor_of


def centred(own_key, extent, width, bound, shards=(), held_as=jnp.bfloat16):
    entries = jax.random.normal(own_key, extent, jnp.float32) * width
    if len(shards) > 0:
        entries = shard_levels(own_key, extent, shards, -0.22, 0.18) * entries
    return jnp.clip(entries, min=-bound, max=bound).astype(held_as)


def setup_inputs(seed: int = 0) -> dict:
    key_of = jax.random.split(jax.random.key(seed), 5)
    return {
        "tokens": draw_tokens(jax.random.fold_in(key_of[4], 71), 0),
        "cotangent": draw_cotangent(jax.random.fold_in(key_of[4], 71), 0),
        "weight": draw_weight(jax.random.fold_in(key_of[4], 71), 0),
        "left_vector": centred(key_of[3], (D,), 1.0, 6.0, ((0, 32),), jnp.float32),
    }


epsilon = 1e-06

def reference(tokens, cotangent, weight, left_vector):
    highest = lax.Precision.HIGHEST
    weight_wide = weight.astype(jnp.float32)
    right_raw = jnp.dot(left_vector, weight_wide, precision=highest)
    right_next = right_raw / jnp.sqrt(jnp.sum(right_raw * right_raw) + epsilon)
    left_raw = jnp.dot(weight_wide, right_next, precision=highest)
    left_sq = jnp.sum(left_raw * left_raw)
    spectral = jnp.sqrt(left_sq + epsilon)
    left_next = left_raw / spectral
    block_count = TOKENS // TOK_DEV
    tok_blocks = tokens.reshape(block_count, TOK_DEV, D)
    cot_blocks = cotangent.reshape(block_count, TOK_DEV, OUT)

    def accumulate(running, pieces):
        tok_block, cot_block = pieces
        out_block = (jnp.dot(tok_block, weight, preferred_element_type=jnp.float32) / spectral).astype(jnp.bfloat16)
        back_prod = lax.dot_general(cot_block, weight, (((1,), (1,)), ((), ())), preferred_element_type=jnp.float32)
        back_block = (back_prod / spectral).astype(jnp.bfloat16)
        term_block = lax.dot_general(tok_block, cot_block, (((0,), (0,)), ((), ())), preferred_element_type=jnp.float32)
        term_block = lax.optimization_barrier(term_block.astype(jnp.bfloat16)).astype(jnp.float32)
        return (running + term_block, (out_block, back_block))
    grad_sum, (out_all, back_all) = lax.scan(accumulate, jnp.zeros((D, OUT), jnp.float32), (tok_blocks, cot_blocks))
    inner_prod = jnp.sum(grad_sum * weight_wide)
    rank_coeff = inner_prod / (spectral * spectral)
    gradient = grad_sum / spectral - rank_coeff * left_next[:, None] * right_next[None, :]
    grad_rms = jnp.sqrt(jnp.mean(gradient * gradient) + epsilon)
    update = (gradient / grad_rms).astype(jnp.bfloat16)
    layer_out = out_all.reshape(TOKENS, OUT)
    input_grad = back_all.reshape(TOKENS, D)
    return (layer_out, input_grad, update, left_next, right_next)
```

```python
import jax
import jax.numpy as jnp
from jax import lax
from jax.experimental import pallas as pl
from jax.experimental.pallas import tpu as pltpu
from jax.sharding import Mesh
from jax.sharding import PartitionSpec as P

MESH = pl.DeviceIdType.MESH
BF, F32 = jnp.bfloat16, jnp.float32
EPS = 1e-06
ENTRIES = 4096 * 2048

FSDP = ("fx", "fy", "fc")
FSDP_DP = ("fx", "fy", "fc", "dp")
SIZE = {"fx": 4, "fy": 4, "fc": 2, "dp": 4}
ORDER = (("dp", "fx", "fy"), ("dp", "fy", "fx"), ("fx", "fy", "dp"), ("fy", "fx", "dp"))


def kernel(
    tok, cot, w, lv, lo, ig, up, ln_ref, rn_ref,
    W, T, TP, C, CP, D, R1, R2, E, Q1, Q2, F, R3, G, GA, LO, IG, UP,
    prc, prx, pry, sqc, sqx, sqy, nmc, nmx, nmy, nmz, scal,
    ag_s, ag_r, fw_s, fw_r, ex_s, ex_r, rs_s, rs_r, p3_s, p3_r, gz_s, gz_r,
    pr_s, pr_r, sq_s, sq_r, nm_s, nm_r, ld_w, ld_c, ld_t, st,
):
    pos = {name: lax.axis_index(name) for name in SIZE}
    mx, my, mc, mz = (pos[name] for name in ("fx", "fy", "fc", "dp"))
    oc = 1 - mc

    def peer(name, step):
        return {name: (pos[name] + step) % SIZE[name]}

    def copy_to(src, dst, s, r, dev):
        return pltpu.make_async_remote_copy(
            src_ref=src, dst_ref=dst, send_sem=s, recv_sem=r, device_id=dev, device_id_type=MESH
        )

    def arrived(dst, sem):
        pltpu.make_async_copy(dst, dst, sem).wait()

    sent = []

    def started(copy):
        copy.start()

    half = (pl.ds(0, 1024), pl.ds(1024, 1024))
    first, second = ("fx", "fy"), ("fy", "fx")

    def block(h, a1, a2, rows=slice(None)):
        xy = (a1, a2) if h == 0 else (a2, a1)
        return W.at[mc, xy[0], xy[1], rows, half[h]]

    top, bottom = pl.ds(0, 64), pl.ds(64, 64)
    gather = {}
    landed = {}
    for h in range(2):
        n1, n2 = first[h], second[h]
        m1, m2 = pos[n1], pos[n2]
        for op in range(5):
            if op == 0:
                name, at = n1, lambda step, rows=slice(None), h=h, m1=m1, m2=m2: block(h, (m1 + step) % 4, m2, rows)
            else:
                col = (m1 + (0, 3, 1, 2)[op - 1]) % 4
                name, at = n2, lambda step, rows=slice(None), h=h, col=col, m2=m2: block(h, col, (m2 + step) % 4, rows)
            plus, minus = peer(name, 1), peer(name, 3)
            src = (at(0), at(0), at(3, top), at(1, bottom))
            for e, dev in enumerate((plus, minus, plus, minus)):
                gather[h, op, e] = copy_to(src[e], src[e], ag_s.at[h, op, e], ag_r.at[h, op, e], dev)
            got = (at(3), at(1), at(2, top), at(2, bottom))
            for e in range(4):
                landed[h, op, e] = (got[e], ag_r.at[h, op, e])
    partner = peer("fc", 1)
    across, crossed = {}, {}
    for h in range(2):
        for slot in range(4):
            col = (pos[first[h]] + (0, 3, 1, 2)[slot]) % 4
            mine = W.at[mc, col, :, :, half[h]] if h == 0 else W.at[mc, :, col, :, half[h]]
            other = W.at[oc, col, :, :, half[h]] if h == 0 else W.at[oc, :, col, :, half[h]]
            across[h, slot] = copy_to(mine, mine, fw_s.at[h, slot], fw_r.at[h, slot], partner)
            crossed[h, slot] = (other, fw_r.at[h, slot])
    give_c = copy_to(C, CP, ex_s.at[4], ex_r.at[4], partner)
    give_t = [
        copy_to(T.at[oc, :, pl.ds(512 * g, 512)], TP.at[:, pl.ds(512 * g, 512)], ex_s.at[g], ex_r.at[g], partner)
        for g in range(4)
    ]

    ring = {}
    for ph, (S, A1, A2) in enumerate(((D, R1, R2), (E, Q1, Q2))):
        for k in range(4):
            name = ORDER[k][ph]
            m = pos[name]
            tp, tm, to = (m + 1) % 4, (m + 3) % 4, (m + 2) % 4
            plus, minus = peer(name, 1), peer(name, 3)
            a, b = pl.ds(0, 2), pl.ds(2, 2)
            moves = (
                (S.at[k, to, a], A1.at[k, 0], plus),
                (S.at[k, to, b], A1.at[k, 1], minus),
                (S.at[k, tp, b], A2.at[k, 0, b], plus),
                (S.at[k, tm, a], A2.at[k, 1, a], minus),
                (S.at[k, tp, a], A2.at[k, 0, a], plus),
                (S.at[k, tm, b], A2.at[k, 1, b], minus),
            )
            for e, (src, dst, dev) in enumerate(moves):
                ring[ph, k, e] = copy_to(src, dst, rs_s.at[ph, k, e], rs_r.at[ph, k, e], dev)
            ring[ph, k, "at"] = (m, tp, tm)
    last = {}
    for k in range(4):
        name = ORDER[k][2]
        for j in range(1, 4):
            to = (pos[name] + j) % 4
            last[k, j] = copy_to(F.at[k, to], R3.at[k, j - 1], p3_s.at[k, j - 1], p3_r.at[k, j - 1], {name: to})
    share = [
        copy_to(GA.at[mz], GA.at[mz], gz_s.at[j - 1], gz_r.at[j - 1], peer("dp", j)) for j in range(1, 4)
    ]

    def exchange(buf, name, s, r, base):
        m, n = pos[name], SIZE[name]
        return [
            (
                copy_to(buf.at[m], buf.at[m], s.at[base + j - 1], r.at[base + j - 1], peer(name, j)),
                buf.at[(m + n - j) % n],
                r.at[base + j - 1],
            )
            for j in range(1, n)
        ]

    small = {
        "pr0": exchange(prc, "fc", pr_s, pr_r, 0),
        "pr1": exchange(prx, "fx", pr_s, pr_r, 1),
        "pr2": exchange(pry, "fy", pr_s, pr_r, 4),
        "sq0": exchange(sqc, "fc", sq_s, sq_r, 0),
        "sq1": exchange(sqx, "fx", sq_s, sq_r, 1),
        "sq2": exchange(sqy, "fy", sq_s, sq_r, 4),
        "nm0": exchange(nmc, "fc", nm_s, nm_r, 0),
        "nm1": exchange(nmx, "fx", nm_s, nm_r, 1),
        "nm2": exchange(nmy, "fy", nm_s, nm_r, 4),
        "nm3": exchange(nmz, "dp", nm_s, nm_r, 7),
    }

    def put(key, buf, name, value):
        buf[pos[name]] = value
        for copy, _, _ in small[key]:
            copy.start()

    def total(key, buf):
        for _, dst, sem in small[key]:
            arrived(dst, sem)
        value = buf[0]
        for j in range(1, buf.shape[0]):
            value = value + buf[j]
        return value

    load_w = pltpu.make_async_copy(w, W.at[mc, mx, my], ld_w)
    load_w.start()
    load_c = pltpu.make_async_copy(cot, C, ld_c)
    load_c.start()
    for p in range(2):
        side = (oc + p) % 2
        for b in range(16):
            pltpu.make_async_copy(
                tok.at[:, pl.ds(pl.multiple_of((2 * b + side) * 128, 128), 128)],
                T.at[side, :, pl.ds(128 * b, 128)],
                ld_t.at[p, b // 4],
            ).start()

    def loaded(p, g):
        side = (oc + p) % 2
        region = T.at[side, :, pl.ds(512 * g, 512)]
        pltpu.make_async_copy(region, region, ld_t.at[p, g]).wait()

    barrier = pltpu.get_barrier_semaphore()
    for name, n in SIZE.items():
        for j in range(1, n):
            pl.semaphore_signal(barrier, inc=1, device_id=peer(name, j), device_id_type=MESH)
    pl.semaphore_wait(barrier, 10)

    load_w.wait()
    for h in range(2):
        for op in (0, 1):
            gather[h, op, 0].start()
            gather[h, op, 1].start()
    load_c.wait()
    give_c.start()
    w_wide = W[mc, mx, my].astype(F32)
    lv_col = jnp.broadcast_to(lv[...], (128, 128)).T[:, 0:1]
    put("pr0", prc, "fc", jnp.sum(w_wide * lv_col, axis=0, keepdims=True))
    for g in range(4):
        loaded(0, g)
        give_t[g].start()

    def forward(h, op):
        arrived(*landed[h, op, 0])
        gather[h, op, 2].start()
        arrived(*landed[h, op, 1])
        gather[h, op, 3].start()

    def spread(h, op):
        gather[h, op, 0].start()
        gather[h, op, 1].start()

    def cross(h, slot):
        arrived(*landed[h, slot + 1, 2])
        arrived(*landed[h, slot + 1, 3])
        across[h, slot].start()

    forward(0, 0)
    forward(1, 0)
    for op in (2, 3):
        for h in range(2):
            spread(h, op)

    def ring_go(ph, k, *events):
        for e in events:
            ring[ph, k, e].start()

    def ring_mid(ph, k):
        S, A1 = ((D, R1), (E, Q1))[ph]
        _, tp, tm = ring[ph, k, "at"]
        for d, (t, lo_, e) in enumerate(((tp, 0, 4), (tm, 2, 5))):
            arrived(A1.at[k, d], rs_r.at[ph, k, d])
            for i in range(2):
                S[k, t, lo_ + i] = (S[k, t, lo_ + i].astype(F32) + A1[k, d, i].astype(F32)).astype(BF)
            ring[ph, k, e].start()

    def ring_end(ph, k):
        S, A2, out = ((D, R2, E), (E, Q2, F))[ph]
        m = ring[ph, k, "at"][0]
        a, b = pl.ds(0, 2), pl.ds(2, 2)
        arrived(A2.at[k, 0, b], rs_r.at[ph, k, 2])
        arrived(A2.at[k, 1, a], rs_r.at[ph, k, 3])
        arrived(A2.at[k, 0, a], rs_r.at[ph, k, 4])
        arrived(A2.at[k, 1, b], rs_r.at[ph, k, 5])
        for i in range(4):
            out[k, i] = (
                S[k, m, i].astype(F32) + A2[k, 0, i].astype(F32) + A2[k, 1, i].astype(F32)
            ).astype(BF)

    arrived(CP, ex_r.at[4])
    for g in range(4):
        arrived(TP.at[:, pl.ds(512 * g, 512)], ex_r.at[g])
        loaded(1, g)

    over_tokens = (((0,), (0,)), ((), ()))

    def pr_step1():
        put("pr1", prx, "fx", total("pr0", prc))

    def pr_step2():
        put("pr2", pry, "fy", total("pr1", prx))

    def term(i, carry):
        turn = i // 4
        x = i % 4
        q = (mz + 6 - turn) % 4
        cs = pl.ds(pl.multiple_of(q * 512, 512), 512)
        ms = pl.ds(pl.multiple_of(x * 512, 512), 512)
        r = lax.dot_general(T[mc, :, ms], C[:, cs], over_tokens, preferred_element_type=F32)
        r = r + lax.dot_general(TP[:, ms], CP[:, cs], over_tokens, preferred_element_type=F32)
        r = r.astype(BF)
        for y in range(4):
            rows = slice(128 * y, 128 * y + 128)
            D[0, q, x, y] = r[rows, 0:128]
            D[1, q, y, x] = r[rows, 128:256]
            D[2, x, y, q] = r[rows, 256:384]
            D[3, y, x, q] = r[rows, 384:512]

        @pl.when(i == 3)
        def _():
            for k in (0, 1):
                ring_go(0, k, 0, 1)
            pr_step1()
            forward(0, 1)
            forward(1, 1)

        @pl.when(i == 7)
        def _():
            for k in (0, 1):
                ring_go(0, k, 2)
            for h in range(2):
                arrived(*landed[h, 0, 2])
                arrived(*landed[h, 0, 3])
                spread(h, 4)

        @pl.when(i == 11)
        def _():
            pr_step2()

        return carry

    lax.fori_loop(0, 16, term, 0)
    for k in (0, 1):
        ring_go(0, k, 3)
    for k in (2, 3):
        ring_go(0, k, 0, 1, 2, 3)
    for op in (2, 3):
        for h in range(2):
            forward(h, op)

    right_raw = total("pr2", pry)
    right_next = right_raw / jnp.sqrt(jnp.sum(right_raw * right_raw) + EPS)
    rn_ref[...] = right_next
    left_raw = jnp.sum(W[mc, mx, my].astype(F32) * right_next, axis=1, keepdims=True)
    put("sq0", sqc, "fc", jnp.broadcast_to(jnp.sum(left_raw * left_raw, keepdims=True), (8, 128)))

    ring_mid(0, 0)
    ring_mid(0, 1)
    put("sq1", sqx, "fx", total("sq0", sqc))
    for h in range(2):
        forward(h, 4)
        cross(h, 0)
    put("sq2", sqy, "fy", total("sq1", sqx))
    for h in range(2):
        cross(h, 1)
        cross(h, 2)
    ring_mid(0, 2)
    ring_mid(0, 3)
    for k in (0, 1):
        ring_end(0, k)
        ring_go(1, k, 0, 1, 2, 3)
    left_sq = total("sq2", sqy)
    scal[0] = left_sq
    scal[1] = 1.0 / jnp.sqrt(left_sq + EPS)
    for h in range(2):
        cross(h, 3)
    for h in range(2):
        for slot in range(4):
            arrived(*crossed[h, slot])

    inv = scal[1][0:1, 0:1]

    def back(i, carry):
        x, p = i // 2, i % 2
        rows = W[p, x].reshape(512, 2048)
        r = lax.dot_general(C[...], rows, (((1,), (1,)), ((), ())), preferred_element_type=F32)
        r = (r * inv).astype(BF)
        for y in range(4):
            at = pl.multiple_of(((x * 4 + y) * 2 + p) * 128, 128)
            IG[:, pl.ds(at, 128)] = r[:, 128 * y : 128 * y + 128]

        @pl.when(p == 1)
        def _():
            cs = pl.ds(pl.multiple_of(x * 1024, 1024), 1024)
            pltpu.make_async_copy(IG.at[:, cs], ig.at[:, cs], st.at[0]).start()

        @pl.when(i == 2)
        def _():
            for k in (2, 3):
                ring_end(0, k)
                ring_go(1, k, 0, 1, 2, 3)

        @pl.when(i == 4)
        def _():
            for k in (0, 1):
                ring_mid(1, k)

        @pl.when(i == 6)
        def _():
            for k in (2, 3):
                ring_mid(1, k)

        return carry

    lax.fori_loop(0, 8, back, 0)

    def p3_go(k):
        for j in range(1, 4):
            last[k, j].start()

    def front(i, carry):
        cs = pl.ds(pl.multiple_of(i * 256, 256), 256)
        r = jnp.dot(T[0], W[0, :, :, :, cs].reshape(2048, 256), preferred_element_type=F32)
        r = r + jnp.dot(T[1], W[1, :, :, :, cs].reshape(2048, 256), preferred_element_type=F32)
        LO[:, cs] = (r * inv).astype(BF)
        pltpu.make_async_copy(LO.at[:, cs], lo.at[:, cs], st.at[1]).start()

        @pl.when(i == 0)
        def _():
            for k in (0, 1):
                ring_end(1, k)
                p3_go(k)

        @pl.when(i == 2)
        def _():
            for k in (2, 3):
                ring_end(1, k)
                p3_go(k)

        @pl.when(i == 4)
        def _():
            quarter = pl.ds(pl.multiple_of(mz * 512, 512), 512)
            rn = rn_ref[:, quarter]
            wq = W[mc, mx, my, :, quarter].astype(F32)
            raw = jnp.sum(W[mc, mx, my].astype(F32) * rn_ref[...], axis=1, keepdims=True)
            ln = raw * inv
            sums = [jnp.zeros((1, 128), F32)] * 3
            for k in range(4):
                g = F[k, pos[ORDER[k][2]]].astype(F32)
                for j in range(3):
                    arrived(R3.at[k, j], p3_r.at[k, j])
                    g = g + R3[k, j].astype(F32)
                cols = slice(128 * k, 128 * k + 128)
                GA[mz, :, cols] = g.astype(BF)
                sums[0] = sums[0] + jnp.sum(g * g, axis=0, keepdims=True)
                sums[1] = sums[1] + jnp.sum(g * wq[:, cols], axis=0, keepdims=True)
                sums[2] = sums[2] + jnp.sum(g * ln, axis=0, keepdims=True) * rn[:, cols]
            for copy in share:
                copy.start()
            put("nm0", nmc, "fc", jnp.concatenate(sums + [jnp.zeros((5, 128), F32)], axis=0))

        @pl.when(i == 5)
        def _():
            put("nm1", nmx, "fx", total("nm0", nmc))

        @pl.when(i == 6)
        def _():
            put("nm2", nmy, "fy", total("nm1", nmx))

        return carry

    lax.fori_loop(0, 8, front, 0)
    put("nm3", nmz, "dp", total("nm2", nmy))

    sums = jnp.sum(total("nm3", nmz), axis=1, keepdims=True)
    grad_sq_raw, inner, crossed_term = sums[0:1], sums[1:2], sums[2:3]
    lsq = scal[0][0:1, 0:1]
    sq = lsq + EPS
    coeff = inner / sq
    rn = rn_ref[...]
    raw = jnp.sum(W[mc, mx, my].astype(F32) * rn, axis=1, keepdims=True)
    ln = raw * inv
    ln_ref[...] = jnp.broadcast_to(ln, (128, 128)).T[0:1]
    right_unit = jnp.sum(rn * rn, keepdims=True)
    grad_sq = (
        grad_sq_raw / sq - 2.0 * coeff * crossed_term * inv + coeff * coeff * (lsq / sq) * right_unit
    )
    inv_rms = 1.0 / jnp.sqrt(grad_sq / ENTRIES + EPS)
    for j in range(1, 4):
        arrived(GA.at[(mz + 4 - j) % 4], gz_r.at[j - 1])
    scale = inv * inv_rms
    column = ln * (coeff * inv_rms)
    for q in range(4):
        cs = slice(512 * q, 512 * q + 512)
        UP[:, cs] = (GA[q].astype(F32) * scale - column * rn[:, cs]).astype(BF)
    put_up = pltpu.make_async_copy(UP, up, st.at[2])
    put_up.start()

    for copy in gather.values():
        copy.wait_send()
    for copy in across.values():
        copy.wait_send()
    give_c.wait_send()
    for copy in give_t:
        copy.wait_send()
    for key, copy in ring.items():
        if key[2] != "at":
            copy.wait_send()
    for copy in last.values():
        copy.wait_send()
    for copy in share:
        copy.wait_send()
    for copies in small.values():
        for copy, _, _ in copies:
            copy.wait_send()
    pltpu.make_async_copy(IG, ig, st.at[0]).wait()
    pltpu.make_async_copy(LO, lo, st.at[1]).wait()
    put_up.wait()


def per_device(tokens, cotangent, weight, left_vector):
    dma = pltpu.SemaphoreType.DMA
    vm = pltpu.VMEM
    hbm = pl.BlockSpec(memory_space=pl.ANY)
    vmem = pl.BlockSpec(memory_space=pltpu.VMEM)
    unit = (128, 128)
    outs = pl.pallas_call(
        kernel,
        out_shape=(
            jax.ShapeDtypeStruct((512, 2048), BF),
            jax.ShapeDtypeStruct((512, 4096), BF),
            jax.ShapeDtypeStruct((128, 2048), BF),
            jax.ShapeDtypeStruct((1, 128), F32),
            jax.ShapeDtypeStruct((1, 2048), F32),
        ),
        in_specs=[hbm, hbm, hbm, vmem],
        out_specs=(hbm, hbm, hbm, vmem, vmem),
        scratch_shapes=[
            vm((2, 4, 4, 128, 2048), BF),
            vm((2, 512, 2048), BF),
            vm((512, 2048), BF),
            vm((512, 2048), BF),
            vm((512, 2048), BF),
            vm((4, 4, 4, 4, *unit), BF),
            vm((4, 2, 2, 4, *unit), BF),
            vm((4, 2, 4, 4, *unit), BF),
            vm((4, 4, 4, *unit), BF),
            vm((4, 2, 2, *unit), BF),
            vm((4, 2, 4, *unit), BF),
            vm((4, 4, *unit), BF),
            vm((4, 3, *unit), BF),
            vm((8, 128), F32),
            vm((4, 128, 512), BF),
            vm((512, 2048), BF),
            vm((512, 4096), BF),
            vm((128, 2048), BF),
            vm((2, 1, 2048), F32),
            vm((4, 1, 2048), F32),
            vm((4, 1, 2048), F32),
            vm((2, 8, 128), F32),
            vm((4, 8, 128), F32),
            vm((4, 8, 128), F32),
            vm((2, 8, 128), F32),
            vm((4, 8, 128), F32),
            vm((4, 8, 128), F32),
            vm((4, 8, 128), F32),
            vm((2, 8, 128), F32),
            dma((2, 5, 4)),
            dma((2, 5, 4)),
            dma((2, 4)),
            dma((2, 4)),
            dma((5,)),
            dma((5,)),
            dma((2, 4, 6)),
            dma((2, 4, 6)),
            dma((4, 3)),
            dma((4, 3)),
            dma((3,)),
            dma((3,)),
            dma((7,)),
            dma((7,)),
            dma((7,)),
            dma((7,)),
            dma((10,)),
            dma((10,)),
            dma,
            dma,
            dma((2, 4)),
            dma((3,)),
        ],
        compiler_params=pltpu.CompilerParams(
            collective_id=0, has_side_effects=True, vmem_limit_bytes=62 * 2**20
        ),
    )(tokens, cotangent, weight, left_vector.reshape(1, 128))
    layer_out, input_grad, update, left_next, right_next = outs
    return (layer_out, input_grad, update, left_next.reshape(128), right_next.reshape(2048))


def solution(mesh):
    torus = Mesh(mesh.devices.reshape(4, 4, 2, mesh.shape["dp"]), FSDP_DP)
    return jax.shard_map(
        per_device,
        mesh=torus,
        in_specs=(P(FSDP_DP, None), P(FSDP_DP, None), P(FSDP, None), P(FSDP)),
        out_specs=(P(FSDP_DP, None), P(FSDP_DP, None), P(FSDP, None), P(FSDP), P()),
        check_vma=False,
    )
```

```python
import jax
import jax.numpy as jnp
from jax import lax
from jax.experimental import pallas as pl
from jax.experimental.pallas import tpu as pltpu
from jax.sharding import Mesh
from jax.sharding import PartitionSpec as P

MESH = pl.DeviceIdType.MESH
BF, F32 = jnp.bfloat16, jnp.float32
EPS = 1e-06
ENTRIES = 4096 * 2048
OFFSET = (0, 1, 3, 2)
MORE = 32
ROWS = (128 + MORE, 128 - MORE)
PIECES = (
    ((0, 0, 128, 0), (128, 0, MORE, 1)),
    ((0, 0, 128, 2), (128, MORE, MORE, 1)),
    ((0, 0, 64, 3), (64, 2 * MORE, 64 - MORE, 1)),
    ((0, 64, 64, 3), (64, 64 + MORE, 64 - MORE, 1)),
)
PIECES = tuple(tuple(piece for piece in pieces if piece[2]) for pieces in PIECES)

FSDP = ("fx", "fy", "fc")
FSDP_DP = ("fx", "fy", "fc", "dp")
SIZE = {"fx": 4, "fy": 4, "fc": 2, "dp": 4}
ORDER = (("dp", "fx", "fy"), ("dp", "fy", "fx"), ("fx", "fy", "dp"), ("fy", "fx", "dp"))


def kernel(
    tok, cot, w, lv, ACC, IG, UP, ln_ref, rn_ref, inv_ref,
    W, T, TP, C, CP, Da, Db, R1a, R1b, R2a, R2b, Ea, Eb, Q1a, Q1b, Q2a, Q2b, Fa, Fb, R3a, R3b, GA,
    prc, prp, sqc, sqp, nmc, nmp, scal,
    ag_s, ag_r, fw_s, fw_r, ex_s, ex_r, rs_s, rs_r, p3_s, p3_r, gz_s, gz_r,
    c2_s, c2_r, pr_s, pr_r, sq_s, sq_r, nc_s, nc_r, np_s, np_r, ld_w, ld_c, ld_t,
):
    def colours(a, b):
        return [a.at[0], a.at[1], b.at[0], b.at[1]]

    D, R1, R2, E, Q1, Q2, F, R3 = (
        colours(a, b)
        for a, b in (
            (Da, Db), (R1a, R1b), (R2a, R2b), (Ea, Eb), (Q1a, Q1b), (Q2a, Q2b), (Fa, Fb), (R3a, R3b)
        )
    )
    pos = {name: lax.axis_index(name) for name in SIZE}
    mx, my, mc, mz = (pos[name] for name in ("fx", "fy", "fc", "dp"))
    oc = 1 - mc
    m1 = mx + mc * (my - mx)
    m2 = my + mc * (mx - my)

    def peer(name, step):
        return {name: (pos[name] + step) % SIZE[name]}

    def along1(step):
        return {"fx": (mx + oc * step) % 4, "fy": (my + mc * step) % 4}

    def along2(step):
        return {"fx": (mx + mc * step) % 4, "fy": (my + oc * step) % 4}

    def copy_to(src, dst, s, r, dev):
        return pltpu.make_async_remote_copy(
            src_ref=src, dst_ref=dst, send_sem=s, recv_sem=r, device_id=dev, device_id_type=MESH
        )

    def arrived(dst, sem):
        pltpu.make_async_copy(dst, dst, sem).wait()

    top, bottom, whole = pl.ds(0, 64), pl.ds(64, 64), pl.ds(0, 128)
    gather, landed = {}, {}
    for op in range(5):
        if op == 0:
            at = lambda step, rows=whole: W.at[mc, (m1 + step) % 4, m2, rows]
            dev = along1
        else:
            col = (m1 + OFFSET[op - 1]) % 4
            at = lambda step, rows=whole, col=col: W.at[mc, col, (m2 + step) % 4, rows]
            dev = along2
        src = (at(0), at(0), at(3, top), at(1, bottom))
        got = (at(3), at(1), at(2, top), at(2, bottom))
        for e, step in enumerate((1, 3, 1, 3)):
            gather[op, e] = copy_to(src[e], src[e], ag_s.at[op, e], ag_r.at[op, e], dev(step))
            landed[op, e] = (got[e], ag_r.at[op, e])
    partner = peer("fc", 1)
    across, crossed = [], []
    for slot in range(4):
        mine = W.at[mc, (m1 + OFFSET[slot]) % 4]
        across.append(copy_to(mine, mine, fw_s.at[slot], fw_r.at[slot], partner))
        crossed.append((W.at[oc, (m2 + OFFSET[slot]) % 4], fw_r.at[slot]))
    quarters = [pl.ds(pl.multiple_of(((mz + 6 - turn) % 4) * 512, 512), 512) for turn in range(4)]
    give_c = [
        copy_to(C.at[:, cs], CP.at[:, cs], ex_s.at[4 + i], ex_r.at[4 + i], partner)
        for i, cs in enumerate(quarters)
    ]
    give_t = [
        copy_to(T.at[oc, :, pl.ds(512 * g, 512)], TP.at[:, pl.ds(512 * g, 512)], ex_s.at[g], ex_r.at[g], partner)
        for g in range(4)
    ]

    ring = {}
    for ph, (S, A1, A2) in enumerate(((D, R1, R2), (E, Q1, Q2))):
        for k in range(4):
            name = ORDER[k][ph]
            m = pos[name]
            tp, tm, to = (m + 1) % 4, (m + 3) % 4, (m + 2) % 4
            plus, minus = peer(name, 1), peer(name, 3)
            a, b = pl.ds(0, 2), pl.ds(2, 2)
            moves = (
                (S[k].at[to, a], A1[k].at[0], plus),
                (S[k].at[to, b], A1[k].at[1], minus),
                (S[k].at[tp, b], A2[k].at[0, b], plus),
                (S[k].at[tm, a], A2[k].at[1, a], minus),
                (S[k].at[tp, a], A2[k].at[0, a], plus),
                (S[k].at[tm, b], A2[k].at[1, b], minus),
            )
            for e, (src, dst, dev) in enumerate(moves):
                ring[ph, k, e] = copy_to(src, dst, rs_s.at[ph, k, e], rs_r.at[ph, k, e], dev)
            ring[ph, k, "at"] = (m, tp, tm)
    last = {}
    for k in range(4):
        name = ORDER[k][2]
        for j in range(1, 4):
            to = (pos[name] + j) % 4
            last[k, j] = copy_to(F[k].at[to], R3[k].at[j - 1], p3_s.at[k, j - 1], p3_r.at[k, j - 1], {name: to})
    share = [
        copy_to(GA.at[mz], GA.at[mz], gz_s.at[j - 1], gz_r.at[j - 1], peer("dp", j)) for j in range(1, 4)
    ]

    def exchange(buf, s, r, slot_of, devices):
        here = slot_of(0)
        return [
            (copy_to(buf.at[here], buf.at[here], s.at[j], r.at[j], dev), buf.at[slot_of(j + 1)], r.at[j])
            for j, dev in enumerate(devices)
        ]

    plane_steps = [(i // 4, i % 4) for i in range(1, 16)]
    plane = [{"fx": (mx + i) % 4, "fy": (my + j) % 4} for i, j in plane_steps]
    cz_steps = [(i // 4, i % 4) for i in range(1, 8)]
    core_z = [{"fc": (mc + i) % 2, "dp": (mz + j) % 4} for i, j in cz_steps]

    def plane_slot(j):
        return ((mx + 4 - j // 4) % 4) * 4 + (my + 4 - j % 4) % 4

    def cz_slot(j):
        return ((mc + 2 - j // 4) % 2) * 4 + (mz + 4 - j % 4) % 4

    def core_slot(j):
        return (mc + j) % 2

    pr0 = exchange(prc, c2_s.at[pl.ds(0, 1)], c2_r.at[pl.ds(0, 1)], core_slot, [partner])
    pr1 = exchange(prp, pr_s, pr_r, plane_slot, plane)
    sq0 = exchange(sqc, c2_s.at[pl.ds(1, 1)], c2_r.at[pl.ds(1, 1)], core_slot, [partner])
    sq1 = exchange(sqp, sq_s, sq_r, plane_slot, plane)
    nm0 = exchange(nmc, nc_s, nc_r, cz_slot, core_z)
    nm1 = exchange(nmp, np_s, np_r, plane_slot, plane)

    def put(copies, buf, slot, value):
        buf[slot] = value
        for copy, _, _ in copies:
            copy.start()

    def total(copies, buf):
        for _, dst, sem in copies:
            arrived(dst, sem)
        value = buf[0]
        for j in range(1, buf.shape[0]):
            value = value + buf[j]
        return value

    load_w = pltpu.make_async_copy(w, W.at[mc, m1, m2], ld_w)
    load_w.start()
    load_c = pltpu.make_async_copy(cot, C, ld_c)
    load_c.start()
    for p in range(2):
        side = (oc + p) % 2
        for b in range(16):
            xy = b + side * ((b % 4) * 4 + b // 4 - b)
            pltpu.make_async_copy(
                tok.at[:, pl.ds(pl.multiple_of((2 * xy + side) * 128, 128), 128)],
                T.at[side, :, pl.ds(128 * b, 128)],
                ld_t.at[p, b // 4],
            ).start()

    def loaded(p, g):
        side = (oc + p) % 2
        region = T.at[side, :, pl.ds(512 * g, 512)]
        pltpu.make_async_copy(region, region, ld_t.at[p, g]).wait()

    barrier = pltpu.get_barrier_semaphore()
    others = plane + core_z
    for dev in others:
        pl.semaphore_signal(barrier, inc=1, device_id=dev, device_id_type=MESH)
    load_w.wait()
    w_wide = W[mc, m1, m2].astype(F32)
    lv_col = jnp.broadcast_to(lv[...], (128, 128)).T[:, 0:1]
    part_right = jnp.sum(w_wide * lv_col, axis=0, keepdims=True)
    prc[mc] = part_right
    ACC[...] = jnp.zeros((512, 2048), F32)
    pl.semaphore_wait(barrier, len(others))

    def spread(op):
        gather[op, 0].start()
        gather[op, 1].start()

    def forward(op):
        arrived(*landed[op, 0])
        gather[op, 2].start()
        arrived(*landed[op, 1])
        gather[op, 3].start()

    def cross(slot):
        arrived(*landed[slot + 1, 2])
        arrived(*landed[slot + 1, 3])
        across[slot].start()

    def meet():
        arrived(*landed[0, 2])
        arrived(*landed[0, 3])

    for copy, _, _ in pr0:
        copy.start()
    spread(0)
    load_c.wait()
    give_c[0].start()
    for g in range(4):
        loaded(0, g)
        give_t[g].start()
    for copy in give_c[1:]:
        copy.start()
    put(pr1, prp, mx * 4 + my, total(pr0, prc))
    spread(1)

    def ring_go(ph, k, *events):
        for e in events:
            ring[ph, k, e].start()

    def ring_mid(ph, k):
        S, A1 = ((D, R1), (E, Q1))[ph]
        _, tp, tm = ring[ph, k, "at"]
        for d, (t, lo_, e) in enumerate(((tp, 0, 4), (tm, 2, 5))):
            arrived(A1[k].at[d], rs_r.at[ph, k, d])
            for i in range(2):
                S[k][t, lo_ + i] = (S[k][t, lo_ + i].astype(F32) + A1[k][d, i].astype(F32)).astype(BF)
            ring[ph, k, e].start()

    def ring_end(ph, k):
        S, A2, out = ((D, R2, E), (E, Q2, F))[ph]
        m = ring[ph, k, "at"][0]
        a, b = pl.ds(0, 2), pl.ds(2, 2)
        arrived(A2[k].at[0, b], rs_r.at[ph, k, 2])
        arrived(A2[k].at[1, a], rs_r.at[ph, k, 3])
        arrived(A2[k].at[0, a], rs_r.at[ph, k, 4])
        arrived(A2[k].at[1, b], rs_r.at[ph, k, 5])
        for i in range(4):
            out[k][i] = (
                S[k][m, i].astype(F32) + A2[k][0, i].astype(F32) + A2[k][1, i].astype(F32)
            ).astype(BF)

    def p1_end(k):
        ring_end(0, k)
        ring_go(1, k, 0, 1, 2, 3)

    def p2_end(k):
        ring_end(1, k)
        for j in range(1, 4):
            last[k, j].start()

    def sq_start():
        right_raw = total(pr1, prp)
        right_next = right_raw / jnp.sqrt(jnp.sum(right_raw * right_raw) + EPS)
        rn_ref[...] = right_next
        left_raw = jnp.sum(W[mc, m1, m2].astype(F32) * right_next, axis=1, keepdims=True)
        put(sq0, sqc, mc, jnp.broadcast_to(jnp.sum(left_raw * left_raw, keepdims=True), (8, 128)))

    def sq_plane():
        put(sq1, sqp, mx * 4 + my, total(sq0, sqc))

    def sq_end():
        left_sq = total(sq1, sqp)
        scal[0] = left_sq
        inv_ref[...] = 1.0 / jnp.sqrt(left_sq + EPS)

    def wait_c(turn):
        arrived(CP.at[:, quarters[turn]], ex_r.at[4 + turn])

    def wait_t(g):
        arrived(TP.at[:, pl.ds(512 * g, 512)], ex_r.at[g])
        loaded(1, g)

    wait_c(0)
    over_tokens = (((0,), (0,)), ((), ()))

    def run(events, i):
        for when, todo in events.items():
            @pl.when(i == when)
            def _():
                for f, *a in todo:
                    f(*a)

    def term(i, carry):
        turn = i // 4
        g = i % 4
        run(TERM_WAITS, i)
        q = (mz + 6 - turn) % 4
        cs = pl.ds(pl.multiple_of(q * 512, 512), 512)
        ms = pl.ds(pl.multiple_of(g * 512, 512), 512)
        r = lax.dot_general(T[mc, :, ms], C[:, cs], over_tokens, preferred_element_type=F32)
        r = r + lax.dot_general(TP[:, ms], CP[:, cs], over_tokens, preferred_element_type=F32)
        r = r.astype(BF)
        for h in range(4):
            x = g + mc * (h - g)
            y = h + mc * (g - h)
            at = ((q, x, y), (q, y, x), (x, y, q), (y, x, q))
            for k in range(4):
                for u, b, n, tile in PIECES[k]:
                    rows = slice(128 * h + b, 128 * h + b + n)
                    D[k][(*at[k], slice(u, u + n))] = r[rows, 128 * tile : 128 * tile + 128]
        run(TERM_EVENTS, i)
        return carry

    TERM_WAITS = {
        0: [(wait_t, 0)],
        1: [(wait_t, 1)],
        2: [(wait_t, 2)],
        3: [(wait_t, 3)],
        4: [(wait_c, 1)],
        8: [(wait_c, 2)],
        12: [(wait_c, 3)],
    }
    TERM_EVENTS = {
        3: [(ring_go, 0, 0, 0, 1), (ring_go, 0, 1, 0, 1)],
        7: [(ring_go, 0, 0, 2), (ring_go, 0, 1, 2)],
        10: [(forward, 1), (forward, 0), (spread, 2)],
        12: [(sq_start,)],
        14: [(sq_plane,)],
        15: [
            (ring_go, 0, 2, 0, 1, 2, 3), (ring_go, 0, 3, 0, 1, 2, 3),
            (ring_go, 0, 0, 3), (ring_go, 0, 1, 3),
        ],
    }
    lax.fori_loop(0, 16, term, 0)

    def group(slot):
        arrived(*crossed[slot])

    def norms():
        inv = inv_ref[0:1, 0:1]
        quarter = pl.ds(pl.multiple_of(mz * 512, 512), 512)
        rn = rn_ref[:, quarter]
        wq = W[mc, m1, m2, :, quarter].astype(F32)
        raw = jnp.sum(W[mc, m1, m2].astype(F32) * rn_ref[...], axis=1, keepdims=True)
        ln = raw * inv
        sums = [jnp.zeros((1, 128), F32)] * 3
        for k in range(4):
            unit = F[k][pos[ORDER[k][2]]].astype(F32)
            for j in range(3):
                arrived(R3[k].at[j], p3_r.at[k, j])
                unit = unit + R3[k][j].astype(F32)
            for u, b, n, tile in PIECES[k]:
                g, rows, cols = unit[u : u + n], slice(b, b + n), slice(128 * tile, 128 * tile + 128)
                GA[mz, rows, cols] = g.astype(BF)
                sums[0] = sums[0] + jnp.sum(g * g, axis=0, keepdims=True)
                sums[1] = sums[1] + jnp.sum(g * wq[rows, cols], axis=0, keepdims=True)
                sums[2] = sums[2] + jnp.sum(g * ln[rows], axis=0, keepdims=True) * rn[:, cols]
        put(nm0, nmc, mc * 4 + mz, jnp.concatenate(sums + [jnp.zeros((5, 128), F32)], axis=0))
        for copy in share:
            copy.start()

    def nm_plane():
        put(nm1, nmp, mx * 4 + my, total(nm0, nmc))

    def both(s, carry):
        run(BOTH_EVENTS, s)
        early = s < 4
        kind = jnp.where(early, s // 2, s % 2)
        i = jnp.where(early, s % 2, s // 2)
        slot, other = i // 2, i % 2
        off = slot + slot // 2 - 2 * (slot // 3)
        p = (mc + other) % 2
        col = (m1 + other * (m2 - m1) + off) % 4

        @pl.when(kind == 0)
        def _():
            ms = pl.ds(pl.multiple_of(col * 512, 512), 512)
            for n in range(4):
                cs = slice(512 * n, 512 * n + 512)
                rows = W[p, col, :, :, cs].reshape(512, 512)
                ACC[:, cs] = ACC[:, cs] + jnp.dot(T[p, :, ms], rows, preferred_element_type=F32)

        @pl.when(kind == 1)
        def _():
            inv = inv_ref[0:1, 0:1]
            rows = W[p, col].reshape(512, 2048)
            r = lax.dot_general(C[...], rows, (((1,), (1,)), ((), ())), preferred_element_type=F32)
            r = (r * inv).astype(BF)
            for h in range(4):
                x = col + p * (h - col)
                y = h + p * (col - h)
                at = pl.multiple_of(((x * 4 + y) * 2 + p) * 128, 128)
                IG[:, pl.ds(at, 128)] = r[:, 128 * h : 128 * h + 128]

        return carry

    BOTH_EVENTS = {
        0: [(cross, 0)],
        1: [(ring_mid, 0, 0), (ring_mid, 0, 1), (group, 0)],
        2: [(sq_end,)],
        4: [(forward, 2), (ring_mid, 0, 2), (ring_mid, 0, 3), (spread, 3), (meet,), (cross, 1)],
        5: [(p1_end, 2), (p1_end, 3)],
        6: [(group, 1)],
        8: [
            (forward, 3), (p1_end, 0), (p1_end, 1), (spread, 4),
            (ring_mid, 1, 2), (ring_mid, 1, 3), (cross, 2),
        ],
        9: [(ring_mid, 1, 0), (ring_mid, 1, 1)],
        10: [(p2_end, 2), (p2_end, 3), (group, 2)],
        11: [(p2_end, 0), (p2_end, 1)],
        12: [(forward, 4), (norms,), (cross, 3)],
        13: [(nm_plane,)],
        14: [(group, 3)],
    }
    lax.fori_loop(0, 16, both, 0)

    inv = inv_ref[0:1, 0:1]
    sums = jnp.sum(total(nm1, nmp), axis=1, keepdims=True)
    grad_sq_raw, inner, crossed_term = sums[0:1], sums[1:2], sums[2:3]
    lsq = scal[0][0:1, 0:1]
    sq = lsq + EPS
    coeff = inner / sq
    rn = rn_ref[...]
    raw = jnp.sum(W[mc, m1, m2].astype(F32) * rn, axis=1, keepdims=True)
    ln = raw * inv
    ln_ref[...] = jnp.broadcast_to(ln, (128, 128)).T[0:1]
    right_unit = jnp.sum(rn * rn, keepdims=True)
    grad_sq = (
        grad_sq_raw / sq - 2.0 * coeff * crossed_term * inv + coeff * coeff * (lsq / sq) * right_unit
    )
    inv_rms = 1.0 / jnp.sqrt(grad_sq / ENTRIES + EPS)
    for j in range(1, 4):
        arrived(GA.at[(mz + 4 - j) % 4], gz_r.at[j - 1])
    scale = inv * inv_rms
    column = ln * (coeff * inv_rms)
    for q in range(4):
        cs = slice(512 * q, 512 * q + 512)
        UP[:, cs] = (GA[q].astype(F32) * scale - column * rn[:, cs]).astype(BF)

    for copy in list(gather.values()) + across + give_c + give_t + list(last.values()) + share:
        copy.wait_send()
    for key, copy in ring.items():
        if key[2] != "at":
            copy.wait_send()
    for copies in (pr0, pr1, sq0, sq1, nm0, nm1):
        for copy, _, _ in copies:
            copy.wait_send()


def write_out(acc, ig, up, ln, rn, inv, lo_out, ig_out, up_out, ln_out, rn_out, lo, sems):
    copies = [
        pltpu.make_async_copy(src, dst, sems.at[i])
        for i, (src, dst) in enumerate(((ig, ig_out), (up, up_out), (ln, ln_out), (rn, rn_out)))
    ]
    for copy in copies:
        copy.start()
    for n in range(4):
        rows = pl.ds(128 * n, 128)
        lo[rows] = (acc[rows] * inv[0:1, 0:1]).astype(BF)
        copy = pltpu.make_async_copy(lo.at[rows], lo_out.at[rows], sems.at[4 + n])
        copy.start()
        copies.append(copy)
    for copy in copies:
        copy.wait()


def per_device(tokens, cotangent, weight, left_vector):
    dma = pltpu.SemaphoreType.DMA
    vm = pltpu.VMEM
    hbm = pl.BlockSpec(memory_space=pl.ANY)
    vmem = pl.BlockSpec(memory_space=pltpu.VMEM)
    outs = pl.pallas_call(
        kernel,
        out_shape=(
            vm((512, 2048), F32),
            vm((512, 4096), BF),
            vm((128, 2048), BF),
            vm((1, 128), F32),
            vm((1, 2048), F32),
            vm((8, 128), F32),
        ),
        in_specs=[hbm, hbm, hbm, vmem],
        out_specs=(vmem,) * 6,
        scratch_shapes=[
            vm((2, 4, 4, 128, 2048), BF),
            vm((2, 512, 2048), BF),
            vm((512, 2048), BF),
            vm((512, 2048), BF),
            vm((512, 2048), BF),
            *[
                vm((2, *dims, rows, 128), BF)
                for dims in ((4, 4, 4), (2, 2, 4), (2, 4, 4), (4, 4), (2, 2), (2, 4), (4,), (3,))
                for rows in ROWS
            ],
            vm((4, 128, 512), BF),
            vm((2, 1, 2048), F32),
            vm((16, 1, 2048), F32),
            vm((2, 8, 128), F32),
            vm((16, 8, 128), F32),
            vm((8, 8, 128), F32),
            vm((16, 8, 128), F32),
            vm((1, 8, 128), F32),
            dma((5, 4)),
            dma((5, 4)),
            dma((4,)),
            dma((4,)),
            dma((8,)),
            dma((8,)),
            dma((2, 4, 6)),
            dma((2, 4, 6)),
            dma((4, 3)),
            dma((4, 3)),
            dma((3,)),
            dma((3,)),
            dma((2,)),
            dma((2,)),
            dma((15,)),
            dma((15,)),
            dma((15,)),
            dma((15,)),
            dma((7,)),
            dma((7,)),
            dma((15,)),
            dma((15,)),
            dma,
            dma,
            dma((2, 4)),
        ],
        compiler_params=pltpu.CompilerParams(
            collective_id=0, has_side_effects=True, vmem_limit_bytes=50 * 2**20
        ),
    )(tokens, cotangent, weight, left_vector.reshape(1, 128))
    layer_out, input_grad, update, left_next, right_next = pl.pallas_call(
        write_out,
        out_shape=(
            jax.ShapeDtypeStruct((512, 2048), BF),
            jax.ShapeDtypeStruct((512, 4096), BF),
            jax.ShapeDtypeStruct((128, 2048), BF),
            jax.ShapeDtypeStruct((1, 128), F32),
            jax.ShapeDtypeStruct((1, 2048), F32),
        ),
        in_specs=[vmem] * 6,
        out_specs=(hbm,) * 5,
        scratch_shapes=[vm((512, 2048), BF), dma((8,))],
        compiler_params=pltpu.CompilerParams(vmem_limit_bytes=6 * 2**20),
    )(*[pltpu.with_memory_space_constraint(o, pltpu.VMEM) for o in outs])
    return (layer_out, input_grad, update, left_next.reshape(128), right_next.reshape(2048))


def solution(mesh):
    torus = Mesh(mesh.devices.reshape(4, 4, 2, mesh.shape["dp"]), FSDP_DP)
    return jax.shard_map(
        per_device,
        mesh=torus,
        in_specs=(P(FSDP_DP, None), P(FSDP_DP, None), P(FSDP, None), P(FSDP)),
        out_specs=(P(FSDP_DP, None), P(FSDP_DP, None), P(FSDP, None), P(FSDP), P()),
        check_vma=False,
    )
```

```python
import jax
import jax.numpy as jnp
from jax import lax
from jax.experimental import pallas as pl
from jax.experimental.pallas import tpu as pltpu
from jax.sharding import Mesh
from jax.sharding import PartitionSpec as P

MESH = pl.DeviceIdType.MESH
BF, F32 = jnp.bfloat16, jnp.float32
EPS = 1e-06
ENTRIES = 4096 * 2048
OFFSET = (0, 1, 3, 2)
MORE = 32
ROWS = (128 + MORE, 128 - MORE)
PIECES = (
    ((0, 0, 128, 0), (128, 0, MORE, 1)),
    ((0, 0, 128, 2), (128, MORE, MORE, 1)),
    ((0, 0, 64, 3), (64, 2 * MORE, 64 - MORE, 1)),
    ((0, 64, 64, 3), (64, 64 + MORE, 64 - MORE, 1)),
)
PIECES = tuple(tuple(piece for piece in pieces if piece[2]) for pieces in PIECES)

FSDP = ("fx", "fy", "fc")
FSDP_DP = ("fx", "fy", "fc", "dp")
SIZE = {"fx": 4, "fy": 4, "fc": 2, "dp": 4}
ORDER = (("dp", "fx", "fy"), ("dp", "fy", "fx"), ("fx", "fy", "dp"), ("fy", "fx", "dp"))


def kernel(
    tok, cot, w, lv, ACC, IG, UP, ln_ref, rn_ref, inv_ref,
    W, T, TP, C, CP, Da, Db, R1a, R1b, R2a, R2b, Ea, Eb, Q1a, Q1b, Q2a, Q2b, Fa, Fb, R3a, R3b, GA,
    prc, prp, sqc, sqp, nmc, nmp, scal,
    ag_s, ag_r, fw_s, fw_r, ex_s, ex_r, rs_s, rs_r, p3_s, p3_r, gz_s, gz_r,
    sm_s, sm_r, ld_w, ld_c, ld_t,
):
    def colours(a, b):
        return [a.at[0], a.at[1], b.at[0], b.at[1]]

    D, R1, R2, E, Q1, Q2, F, R3 = (
        colours(a, b)
        for a, b in (
            (Da, Db), (R1a, R1b), (R2a, R2b), (Ea, Eb), (Q1a, Q1b), (Q2a, Q2b), (Fa, Fb), (R3a, R3b)
        )
    )
    pos = {name: lax.axis_index(name) for name in SIZE}
    mx, my, mc, mz = (pos[name] for name in ("fx", "fy", "fc", "dp"))
    oc = 1 - mc
    m1 = mx + mc * (my - mx)
    m2 = my + mc * (mx - my)

    def peer(name, step):
        return {name: (pos[name] + step) % SIZE[name]}

    def along1(step):
        return {"fx": (mx + oc * step) % 4, "fy": (my + mc * step) % 4}

    def along2(step):
        return {"fx": (mx + mc * step) % 4, "fy": (my + oc * step) % 4}

    def copy_to(src, dst, s, r, dev):
        return pltpu.make_async_remote_copy(
            src_ref=src, dst_ref=dst, send_sem=s, recv_sem=r, device_id=dev, device_id_type=MESH
        )

    def arrived(dst, sem):
        pltpu.make_async_copy(dst, dst, sem).wait()

    top, bottom, whole = pl.ds(0, 64), pl.ds(64, 64), pl.ds(0, 128)
    gather, landed = {}, {}
    for op in range(5):
        if op == 0:
            at = lambda step, rows=whole: W.at[mc, (m1 + step) % 4, m2, rows]
            dev = along1
        else:
            col = (m1 + OFFSET[op - 1]) % 4
            at = lambda step, rows=whole, col=col: W.at[mc, col, (m2 + step) % 4, rows]
            dev = along2
        src = (at(0), at(0), at(3, top), at(1, bottom))
        got = (at(3), at(1))
        for e, step in enumerate((1, 3, 1, 3)):
            gather[op, e] = copy_to(src[e], src[e], ag_s.at[min(op, 1)], ag_r.at[op, min(e, 2)], dev(step))
        landed[op, 0], landed[op, 1] = (got[0], ag_r.at[op, 0]), (got[1], ag_r.at[op, 1])
        landed[op, 2] = (at(2), ag_r.at[op, 2])
    partner = peer("fc", 1)
    across, crossed = [], []
    for slot in range(3):
        mine = W.at[mc, (m1 + OFFSET[slot]) % 4]
        across.append(copy_to(mine, mine, fw_s.at[0], fw_r.at[slot], partner))
        crossed.append((W.at[oc, (m2 + OFFSET[slot]) % 4], fw_r.at[slot]))
    for step, at in enumerate(OFFSET):
        mine = W.at[mc, (m1 + 2) % 4, (m2 + at) % 4]
        across.append(copy_to(mine, mine, fw_s.at[0], fw_r.at[3 + step], partner))
        crossed.append((W.at[oc, (m2 + 2) % 4, (m1 + at) % 4], fw_r.at[3 + step]))
    quarters = [pl.ds(pl.multiple_of(((mz + 6 - turn) % 4) * 512, 512), 512) for turn in range(4)]
    give_c = [
        copy_to(C.at[:, cs], CP.at[:, cs], ex_s.at[0], ex_r.at[4 + i], partner)
        for i, cs in enumerate(quarters)
    ]
    give_t = [
        copy_to(T.at[oc, :, pl.ds(512 * g, 512)], TP.at[:, pl.ds(512 * g, 512)], ex_s.at[0], ex_r.at[g], partner)
        for g in range(4)
    ]

    ring = {}
    for ph, (S, A1, A2) in enumerate(((D, R1, R2), (E, Q1, Q2))):
        for k in range(4):
            name = ORDER[k][ph]
            m = pos[name]
            tp, tm, to = (m + 1) % 4, (m + 3) % 4, (m + 2) % 4
            plus, minus = peer(name, 1), peer(name, 3)
            a, b = pl.ds(0, 2), pl.ds(2, 2)
            moves = (
                (S[k].at[to, a], A1[k].at[0], plus),
                (S[k].at[to, b], A1[k].at[1], minus),
                (S[k].at[tp, b], A2[k].at[0, b], plus),
                (S[k].at[tm, a], A2[k].at[1, a], minus),
                (S[k].at[tp, a], A2[k].at[0, a], plus),
                (S[k].at[tm, b], A2[k].at[1, b], minus),
            )
            for e, (src, dst, dev) in enumerate(moves):
                ring[ph, k, e] = copy_to(src, dst, rs_s.at[ph, k], rs_r.at[ph, k, min(e, 2)], dev)
            ring[ph, k, "at"] = (m, tp, tm)
    last = {}
    for k in range(4):
        name = ORDER[k][2]
        for j in range(1, 4):
            to = (pos[name] + j) % 4
            last[k, j] = copy_to(F[k].at[to], R3[k].at[j - 1], p3_s.at[k], p3_r.at[k], {name: to})
    share = [
        copy_to(GA.at[mz], GA.at[mz], gz_s.at[0], gz_r.at[0], peer("dp", j)) for j in range(1, 4)
    ]

    def exchange(buf, s, r, here, devices):
        return [copy_to(buf.at[here], buf.at[here], s, r, dev) for dev in devices], r

    plane_steps = [(i // 4, i % 4) for i in range(1, 16)]
    plane = [{"fx": (mx + i) % 4, "fy": (my + j) % 4} for i, j in plane_steps]
    cz_steps = [(i // 4, i % 4) for i in range(1, 8)]
    core_z = [{"fc": (mc + i) % 2, "dp": (mz + j) % 4} for i, j in cz_steps]

    here = mx * 4 + my
    pr0 = exchange(prc, sm_s.at[0], sm_r.at[0], mc, [partner])
    pr1 = exchange(prp, sm_s.at[1], sm_r.at[1], here, plane)
    sq0 = exchange(sqc, sm_s.at[2], sm_r.at[2], mc, [partner])
    sq1 = exchange(sqp, sm_s.at[3], sm_r.at[3], here, plane)
    nm0 = exchange(nmc, sm_s.at[4], sm_r.at[4], mc * 4 + mz, core_z)
    nm1 = exchange(nmp, sm_s.at[5], sm_r.at[5], here, plane)

    def put(copies, buf, slot, value):
        buf[slot] = value
        for copy in copies[0]:
            copy.start()

    def total(copies, buf):
        arrived(buf.at[pl.ds(0, buf.shape[0] - 1)], copies[1])
        value = buf[0]
        for j in range(1, buf.shape[0]):
            value = value + buf[j]
        return value

    load_w = pltpu.make_async_copy(w, W.at[mc, m1, m2], ld_w)
    load_w.start()
    def loaded(p, g):
        side = (oc + p) % 2
        region = T.at[side, :, pl.ds(512 * g, 512)]
        pltpu.make_async_copy(region, region, ld_t.at[p, g]).wait()

    barrier = pltpu.get_barrier_semaphore()
    others = plane + core_z
    for dev in others:
        pl.semaphore_signal(barrier, inc=1, device_id=dev, device_id_type=MESH)
    ACC[...] = jnp.zeros((512, 2048), F32)
    load_w.wait()
    load_c = pltpu.make_async_copy(cot, C, ld_c)
    load_c.start()
    for p in range(2):
        side = (oc + p) % 2
        for b in range(16):
            xy = b + side * ((b % 4) * 4 + b // 4 - b)
            pltpu.make_async_copy(
                tok.at[:, pl.ds(pl.multiple_of((2 * xy + side) * 128, 128), 128)],
                T.at[side, :, pl.ds(128 * b, 128)],
                ld_t.at[p, b // 4],
            ).start()

    w_wide = W[mc, m1, m2].astype(F32)
    lv_col = jnp.broadcast_to(lv[...], (128, 128)).T[:, 0:1]
    part_right = jnp.sum(w_wide * lv_col, axis=0, keepdims=True)
    prc[mc] = part_right
    pl.semaphore_wait(barrier, len(others))

    def spread(op):
        gather[op, 0].start()
        gather[op, 1].start()

    def forward(op):
        arrived(*landed[op, 0])
        gather[op, 2].start()
        arrived(*landed[op, 1])
        gather[op, 3].start()

    def cross(slot):
        arrived(*landed[slot + 1, 2])
        across[slot].start()

    def cross_first():
        for i in (3, 4, 5):
            across[i].start()

    def cross_last():
        arrived(*landed[4, 2])
        across[6].start()

    def meet():
        arrived(*landed[0, 2])

    for copy in pr0[0]:
        copy.start()
    put(pr1, prp, mx * 4 + my, total(pr0, prc))
    spread(0)
    spread(1)
    load_c.wait()
    give_c[0].start()
    for g in range(4):
        loaded(0, g)
        give_t[g].start()
    for copy in give_c[1:]:
        copy.start()

    def ring_go(ph, k, *events):
        for e in events:
            ring[ph, k, e].start()

    def ring_mid(ph, k):
        S, A1 = ((D, R1), (E, Q1))[ph]
        _, tp, tm = ring[ph, k, "at"]
        for d, (t, lo_, e) in enumerate(((tp, 0, 4), (tm, 2, 5))):
            arrived(A1[k].at[d], rs_r.at[ph, k, d])
            for i in range(2):
                S[k][t, lo_ + i] = (S[k][t, lo_ + i].astype(F32) + A1[k][d, i].astype(F32)).astype(BF)
            ring[ph, k, e].start()

    def ring_end(ph, k):
        S, A2, out = ((D, R2, E), (E, Q2, F))[ph]
        m = ring[ph, k, "at"][0]
        arrived(A2[k], rs_r.at[ph, k, 2])
        for i in range(4):
            out[k][i] = (
                S[k][m, i].astype(F32) + A2[k][0, i].astype(F32) + A2[k][1, i].astype(F32)
            ).astype(BF)

    def p1_end(k):
        ring_end(0, k)
        ring_go(1, k, 0, 1, 2, 3)

    def p2_end(k):
        ring_end(1, k)
        for j in range(1, 4):
            last[k, j].start()

    def sq_start():
        right_raw = total(pr1, prp)
        right_next = right_raw / jnp.sqrt(jnp.sum(right_raw * right_raw) + EPS)
        rn_ref[...] = right_next
        left_raw = jnp.sum(W[mc, m1, m2].astype(F32) * right_next, axis=1, keepdims=True)
        put(sq0, sqc, mc, jnp.broadcast_to(jnp.sum(left_raw * left_raw, keepdims=True), (8, 128)))

    def sq_plane():
        put(sq1, sqp, mx * 4 + my, total(sq0, sqc))

    def sq_end():
        left_sq = total(sq1, sqp)
        scal[0] = left_sq
        inv_ref[...] = 1.0 / jnp.sqrt(left_sq + EPS)

    def wait_c(turn):
        arrived(CP.at[:, quarters[turn]], ex_r.at[4 + turn])

    def wait_t(g):
        arrived(TP.at[:, pl.ds(512 * g, 512)], ex_r.at[g])
        loaded(1, g)

    wait_c(0)
    over_tokens = (((0,), (0,)), ((), ()))

    def run(events, i):
        for when, todo in events.items():
            @pl.when(i == when)
            def _():
                for f, *a in todo:
                    f(*a)

    def term(i, carry):
        turn = i // 4
        g = i % 4
        run(TERM_WAITS, i)
        q = (mz + 6 - turn) % 4
        cs = pl.ds(pl.multiple_of(q * 512, 512), 512)
        ms = pl.ds(pl.multiple_of(g * 512, 512), 512)
        r = lax.dot_general(T[mc, :, ms], C[:, cs], over_tokens, preferred_element_type=F32)
        r = r + lax.dot_general(TP[:, ms], CP[:, cs], over_tokens, preferred_element_type=F32)
        r = r.astype(BF)
        for h in range(4):
            x = g + mc * (h - g)
            y = h + mc * (g - h)
            at = ((q, x, y), (q, y, x), (x, y, q), (y, x, q))
            for k in range(4):
                for u, b, n, tile in PIECES[k]:
                    rows = slice(128 * h + b, 128 * h + b + n)
                    D[k][(*at[k], slice(u, u + n))] = r[rows, 128 * tile : 128 * tile + 128]
        run(TERM_EVENTS, i)
        return carry

    TERM_WAITS = {
        0: [(wait_t, 0)],
        1: [(wait_t, 1)],
        2: [(wait_t, 2)],
        3: [(wait_t, 3)],
        4: [(wait_c, 1)],
        8: [(wait_c, 2)],
        12: [(wait_c, 3)],
    }
    TERM_EVENTS = {
        3: [(ring_go, 0, 0, 0, 1), (ring_go, 0, 1, 0, 1)],
        5: [(sq_start,)],
        7: [(ring_go, 0, 0, 2), (ring_go, 0, 1, 2), (sq_plane,)],
        11: [(forward, 1), (forward, 0), (spread, 2)],
        14: [(sq_end,)],
        15: [
            (ring_go, 0, 2, 0, 1, 2, 3), (ring_go, 0, 3, 0, 1, 2, 3),
            (ring_go, 0, 0, 3), (ring_go, 0, 1, 3),
        ],
    }
    lax.fori_loop(0, 16, term, 0)

    def group(slot):
        arrived(*crossed[slot])

    def norms():
        inv = inv_ref[0:1, 0:1]
        quarter = pl.ds(pl.multiple_of(mz * 512, 512), 512)
        rn = rn_ref[:, quarter]
        wq = W[mc, m1, m2, :, quarter].astype(F32)
        raw = jnp.sum(W[mc, m1, m2].astype(F32) * rn_ref[...], axis=1, keepdims=True)
        ln = raw * inv
        sums = [jnp.zeros((1, 128), F32)] * 3
        for k in range(4):
            unit = F[k][pos[ORDER[k][2]]].astype(F32)
            arrived(R3[k], p3_r.at[k])
            for j in range(3):
                unit = unit + R3[k][j].astype(F32)
            for u, b, n, tile in PIECES[k]:
                g, rows, cols = unit[u : u + n], slice(b, b + n), slice(128 * tile, 128 * tile + 128)
                GA[mz, rows, cols] = g.astype(BF)
                sums[0] = sums[0] + jnp.sum(g * g, axis=0, keepdims=True)
                sums[1] = sums[1] + jnp.sum(g * wq[rows, cols], axis=0, keepdims=True)
                sums[2] = sums[2] + jnp.sum(g * ln[rows], axis=0, keepdims=True) * rn[:, cols]
        put(nm0, nmc, mc * 4 + mz, jnp.concatenate(sums + [jnp.zeros((5, 128), F32)], axis=0))
        for copy in share:
            copy.start()

    def nm_plane():
        put(nm1, nmp, mx * 4 + my, total(nm0, nmc))

    def both(s, carry):
        run(BOTH_EVENTS, s)
        kind, i = s % 2, s // 2
        slot, other = i // 2, i % 2
        off = slot + slot // 2 - 2 * (slot // 3)
        p = (mc + other) % 2
        col = (m1 + other * (m2 - m1) + off) % 4

        @pl.when(kind == 0)
        def _():
            ms = pl.ds(pl.multiple_of(col * 512, 512), 512)
            for n in range(4):
                cs = slice(512 * n, 512 * n + 512)
                rows = W[p, col, :, :, cs].reshape(512, 512)
                ACC[:, cs] = ACC[:, cs] + jnp.dot(T[p, :, ms], rows, preferred_element_type=F32)

        @pl.when(kind == 1)
        def _():
            inv = inv_ref[0:1, 0:1]
            rows = W[p, col].reshape(512, 2048)
            r = lax.dot_general(C[...], rows, (((1,), (1,)), ((), ())), preferred_element_type=F32)
            r = (r * inv).astype(BF)
            for h in range(4):
                x = col + p * (h - col)
                y = h + p * (col - h)
                at = pl.multiple_of(((x * 4 + y) * 2 + p) * 128, 128)
                IG[:, pl.ds(at, 128)] = r[:, 128 * h : 128 * h + 128]

        return carry

    BOTH_EVENTS = {
        0: [(cross, 0)],
        2: [(group, 0)],
        3: [(ring_mid, 0, 0), (ring_mid, 0, 1)],
        4: [(forward, 2), (ring_mid, 0, 2), (ring_mid, 0, 3), (spread, 3), (meet,), (cross, 1)],
        6: [(group, 1)],
        7: [(p1_end, 2), (p1_end, 3)],
        8: [
            (p1_end, 0), (p1_end, 1), (forward, 3),
            (ring_mid, 1, 2), (ring_mid, 1, 3), (ring_mid, 1, 0), (ring_mid, 1, 1),
            (spread, 4), (cross, 2),
        ],
        10: [(p2_end, 2), (p2_end, 3), (p2_end, 0), (p2_end, 1), (group, 2)],
    }
    lax.fori_loop(0, 12, both, 0)

    def halves(s, carry):
        run(HALF_EVENTS, s)
        kind, other, late = s % 2, (s // 2) % 2, s // 4
        p = (mc + other) % 2
        a1 = (m1 + other * (m2 - m1) + 2) % 4
        base = m2 + other * (m1 - m2)
        a2 = ((base + 3 * late) % 4, (base + 1 + late) % 4)

        @pl.when(kind == 0)
        def _():
            cols = [T[p, :, pl.ds(pl.multiple_of((a1 * 4 + v) * 128, 128), 128)] for v in a2]
            toks = jnp.concatenate(cols, axis=1)
            for n in range(4):
                cs = slice(512 * n, 512 * n + 512)
                rows = jnp.concatenate([W[p, a1, v, :, cs] for v in a2], axis=0)
                ACC[:, cs] = ACC[:, cs] + jnp.dot(toks, rows, preferred_element_type=F32)

        @pl.when(kind == 1)
        def _():
            inv = inv_ref[0:1, 0:1]
            rows = jnp.concatenate([W[p, a1, v] for v in a2], axis=0)
            r = lax.dot_general(C[...], rows, (((1,), (1,)), ((), ())), preferred_element_type=F32)
            r = (r * inv).astype(BF)
            for h, v in enumerate(a2):
                x = a1 + p * (v - a1)
                y = v + p * (a1 - v)
                at = pl.multiple_of(((x * 4 + y) * 2 + p) * 128, 128)
                IG[:, pl.ds(at, 128)] = r[:, 128 * h : 128 * h + 128]

        return carry

    HALF_EVENTS = {
        0: [(forward, 4), (cross_first,)],
        2: [(norms,), (group, 3), (group, 4)],
        4: [(nm_plane,), (cross_last,)],
        6: [(group, 5), (group, 6)],
    }
    lax.fori_loop(0, 8, halves, 0)

    inv = inv_ref[0:1, 0:1]
    sums = jnp.sum(total(nm1, nmp), axis=1, keepdims=True)
    grad_sq_raw, inner, crossed_term = sums[0:1], sums[1:2], sums[2:3]
    lsq = scal[0][0:1, 0:1]
    sq = lsq + EPS
    coeff = inner / sq
    rn = rn_ref[...]
    raw = jnp.sum(W[mc, m1, m2].astype(F32) * rn, axis=1, keepdims=True)
    ln = raw * inv
    ln_ref[...] = jnp.broadcast_to(ln, (128, 128)).T[0:1]
    right_unit = jnp.sum(rn * rn, keepdims=True)
    grad_sq = (
        grad_sq_raw / sq - 2.0 * coeff * crossed_term * inv + coeff * coeff * (lsq / sq) * right_unit
    )
    inv_rms = 1.0 / jnp.sqrt(grad_sq / ENTRIES + EPS)
    arrived(GA.at[pl.ds(0, 3)], gz_r.at[0])
    scale = inv * inv_rms
    column = ln * (coeff * inv_rms)
    for q in range(4):
        cs = slice(512 * q, 512 * q + 512)
        UP[:, cs] = (GA[q].astype(F32) * scale - column * rn[:, cs]).astype(BF)

    def left(size_of, sem):
        pltpu.make_async_copy(size_of, size_of, sem).wait()

    left(W.at[0, 0, pl.ds(0, 3)], ag_s.at[0])
    left(W.at[0, pl.ds(0, 3)], ag_s.at[1])
    left(W.at[0], fw_s.at[0])
    left(T, ex_s.at[0])
    for k in range(4):
        left(D[k].at[pl.ds(0, 3)], rs_s.at[0, k])
        left(E[k].at[pl.ds(0, 3)], rs_s.at[1, k])
        left(F[k].at[pl.ds(0, 3)], p3_s.at[k])
    left(GA.at[pl.ds(0, 3)], gz_s.at[0])
    for i, buf in enumerate((prc, prp, sqc, sqp, nmc, nmp)):
        left(buf.at[pl.ds(0, buf.shape[0] - 1)], sm_s.at[i])


def write_out(acc, ig, up, ln, rn, inv, lo_out, ig_out, up_out, ln_out, rn_out, lo, sems):
    copies = [
        pltpu.make_async_copy(src, dst, sems.at[i])
        for i, (src, dst) in enumerate(((ig, ig_out), (up, up_out), (ln, ln_out), (rn, rn_out)))
    ]
    for copy in copies:
        copy.start()
    for n in range(4):
        rows = pl.ds(128 * n, 128)
        lo[rows] = (acc[rows] * inv[0:1, 0:1]).astype(BF)
        copy = pltpu.make_async_copy(lo.at[rows], lo_out.at[rows], sems.at[4 + n])
        copy.start()
        copies.append(copy)
    for copy in copies:
        copy.wait()


def per_device(tokens, cotangent, weight, left_vector):
    dma = pltpu.SemaphoreType.DMA
    vm = pltpu.VMEM
    hbm = pl.BlockSpec(memory_space=pl.ANY)
    vmem = pl.BlockSpec(memory_space=pltpu.VMEM)
    outs = pl.pallas_call(
        kernel,
        out_shape=(
            vm((512, 2048), F32),
            vm((512, 4096), BF),
            vm((128, 2048), BF),
            vm((1, 128), F32),
            vm((1, 2048), F32),
            vm((8, 128), F32),
        ),
        in_specs=[hbm, hbm, hbm, vmem],
        out_specs=(vmem,) * 6,
        scratch_shapes=[
            vm((2, 4, 4, 128, 2048), BF),
            vm((2, 512, 2048), BF),
            vm((512, 2048), BF),
            vm((512, 2048), BF),
            vm((512, 2048), BF),
            *[
                vm((2, *dims, rows, 128), BF)
                for dims in ((4, 4, 4), (2, 2, 4), (2, 4, 4), (4, 4), (2, 2), (2, 4), (4,), (3,))
                for rows in ROWS
            ],
            vm((4, 128, 512), BF),
            vm((2, 1, 2048), F32),
            vm((16, 1, 2048), F32),
            vm((2, 8, 128), F32),
            vm((16, 8, 128), F32),
            vm((8, 8, 128), F32),
            vm((16, 8, 128), F32),
            vm((1, 8, 128), F32),
            dma((2,)),
            dma((5, 3)),
            dma((1,)),
            dma((7,)),
            dma((1,)),
            dma((8,)),
            dma((2, 4)),
            dma((2, 4, 3)),
            dma((4,)),
            dma((4,)),
            dma((1,)),
            dma((1,)),
            dma((6,)),
            dma((6,)),
            dma,
            dma,
            dma((2, 4)),
        ],
        compiler_params=pltpu.CompilerParams(
            collective_id=0, has_side_effects=True, vmem_limit_bytes=50 * 2**20
        ),
    )(tokens, cotangent, weight, left_vector.reshape(1, 128))
    layer_out, input_grad, update, left_next, right_next = pl.pallas_call(
        write_out,
        out_shape=(
            jax.ShapeDtypeStruct((512, 2048), BF),
            jax.ShapeDtypeStruct((512, 4096), BF),
            jax.ShapeDtypeStruct((128, 2048), BF),
            jax.ShapeDtypeStruct((1, 128), F32),
            jax.ShapeDtypeStruct((1, 2048), F32),
        ),
        in_specs=[vmem] * 6,
        out_specs=(hbm,) * 5,
        scratch_shapes=[vm((512, 2048), BF), dma((8,))],
        compiler_params=pltpu.CompilerParams(vmem_limit_bytes=6 * 2**20),
    )(*[pltpu.with_memory_space_constraint(o, pltpu.VMEM) for o in outs])
    return (layer_out, input_grad, update, left_next.reshape(128), right_next.reshape(2048))


def solution(mesh):
    torus = Mesh(mesh.devices.reshape(4, 4, 2, mesh.shape["dp"]), FSDP_DP)
    return jax.shard_map(
        per_device,
        mesh=torus,
        in_specs=(P(FSDP_DP, None), P(FSDP_DP, None), P(FSDP, None), P(FSDP)),
        out_specs=(P(FSDP_DP, None), P(FSDP_DP, None), P(FSDP, None), P(FSDP), P()),
        check_vma=False,
    )
```

```python
import jax
import jax.numpy as jnp
from jax import lax
from jax.experimental import pallas as pl
from jax.experimental.pallas import tpu as pltpu
from jax.sharding import Mesh
from jax.sharding import PartitionSpec as P

MESH = pl.DeviceIdType.MESH
BF, F32 = jnp.bfloat16, jnp.float32
EPS = 1e-06
ENTRIES = 4096 * 2048
OFFSET = (0, 1, 3, 2)
MORE = 32
ROWS = (128 + MORE, 128 - MORE)
PIECES = (
    ((0, 0, 128, 0), (128, 0, MORE, 1)),
    ((0, 0, 128, 2), (128, MORE, MORE, 1)),
    ((0, 0, 64, 3), (64, 2 * MORE, 64 - MORE, 1)),
    ((0, 64, 64, 3), (64, 64 + MORE, 64 - MORE, 1)),
)
PIECES = tuple(tuple(piece for piece in pieces if piece[2]) for pieces in PIECES)

FSDP = ("fx", "fy", "fc")
FSDP_DP = ("fx", "fy", "fc", "dp")
SIZE = {"fx": 4, "fy": 4, "fc": 2, "dp": 4}
ORDER = (("dp", "fx", "fy"), ("dp", "fy", "fx"), ("fx", "fy", "dp"), ("fy", "fx", "dp"))


def kernel(
    tok, cot, w, lv, ACC, IG, UP, ln_ref, rn_ref, inv_ref,
    W, T, TP, C, CP, Da, Db, R1a, R1b, R2a, R2b, Ea, Eb, Q1a, Q1b, Q2a, Q2b, Fa, Fb, R3a, R3b, GA,
    prc, prp, sqc, sqp, nmc, nmp, scal,
    ag_s, ag_r, fw_s, fw_r, ex_s, ex_r, rs_s, rs_r, p3_s, p3_r, gz_s, gz_r,
    sm_s, sm_r, ld_w, ld_c, ld_t,
):
    def colours(a, b):
        return [a.at[0], a.at[1], b.at[0], b.at[1]]

    D, R1, R2, E, Q1, Q2, F, R3 = (
        colours(a, b)
        for a, b in (
            (Da, Db), (R1a, R1b), (R2a, R2b), (Ea, Eb), (Q1a, Q1b), (Q2a, Q2b), (Fa, Fb), (R3a, R3b)
        )
    )
    pos = {name: lax.axis_index(name) for name in SIZE}
    mx, my, mc, mz = (pos[name] for name in ("fx", "fy", "fc", "dp"))
    oc = 1 - mc
    m1 = mx + mc * (my - mx)
    m2 = my + mc * (mx - my)

    def peer(name, step):
        return {name: (pos[name] + step) % SIZE[name]}

    def along1(step):
        return {"fx": (mx + oc * step) % 4, "fy": (my + mc * step) % 4}

    def along2(step):
        return {"fx": (mx + mc * step) % 4, "fy": (my + oc * step) % 4}

    def copy_to(src, dst, s, r, dev):
        return pltpu.make_async_remote_copy(
            src_ref=src, dst_ref=dst, send_sem=s, recv_sem=r, device_id=dev, device_id_type=MESH
        )

    def arrived(dst, sem):
        pltpu.make_async_copy(dst, dst, sem).wait()

    top, bottom, whole = pl.ds(0, 64), pl.ds(64, 64), pl.ds(0, 128)
    gather, landed = {}, {}
    for op in range(5):
        if op == 0:
            at = lambda step, rows=whole: W.at[mc, (m1 + step) % 4, m2, rows]
            dev = along1
        else:
            col = (m1 + OFFSET[op - 1]) % 4
            at = lambda step, rows=whole, col=col: W.at[mc, col, (m2 + step) % 4, rows]
            dev = along2
        moves = (
            (at(0, top), 1, 0), (at(0, bottom), 3, 1), (at(0, bottom), 1, 3), (at(0, top), 3, 4),
            (at(3, top), 1, 2), (at(1, bottom), 3, 2),
        )
        for e, (src, step, r) in enumerate(moves):
            gather[op, e] = copy_to(src, src, ag_s.at[min(op, 1)], ag_r.at[op, r], dev(step))
        for r, got in enumerate((at(3, top), at(1, bottom), at(2), at(3, bottom), at(1, top))):
            landed[op, r] = (got, ag_r.at[op, r])
    partner = peer("fc", 1)
    across, crossed = [], []
    for slot in range(3):
        mine = W.at[mc, (m1 + OFFSET[slot]) % 4]
        across.append(copy_to(mine, mine, fw_s.at[0], fw_r.at[slot], partner))
        crossed.append((W.at[oc, (m2 + OFFSET[slot]) % 4], fw_r.at[slot]))
    for step, at in enumerate(OFFSET):
        mine = W.at[mc, (m1 + 2) % 4, (m2 + at) % 4]
        across.append(copy_to(mine, mine, fw_s.at[0], fw_r.at[3 + step], partner))
        crossed.append((W.at[oc, (m2 + 2) % 4, (m1 + at) % 4], fw_r.at[3 + step]))
    quarters = [pl.ds(pl.multiple_of(((mz + 6 - turn) % 4) * 512, 512), 512) for turn in range(4)]
    give_c = [
        copy_to(C.at[:, cs], CP.at[:, cs], ex_s.at[0], ex_r.at[4 + i], partner)
        for i, cs in enumerate(quarters)
    ]
    give_t = [
        copy_to(T.at[oc, :, pl.ds(512 * g, 512)], TP.at[:, pl.ds(512 * g, 512)], ex_s.at[0], ex_r.at[g], partner)
        for g in range(4)
    ]

    ring = {}
    for ph, (S, A1, A2) in enumerate(((D, R1, R2), (E, Q1, Q2))):
        for k in range(4):
            name = ORDER[k][ph]
            m = pos[name]
            tp, tm, to = (m + 1) % 4, (m + 3) % 4, (m + 2) % 4
            plus, minus = peer(name, 1), peer(name, 3)
            a, b = pl.ds(0, 2), pl.ds(2, 2)
            moves = (
                (S[k].at[to, a], A1[k].at[0], plus),
                (S[k].at[to, b], A1[k].at[1], minus),
                (S[k].at[tp, b], A2[k].at[0, b], plus),
                (S[k].at[tm, a], A2[k].at[1, a], minus),
                (S[k].at[tp, a], A2[k].at[0, a], plus),
                (S[k].at[tm, b], A2[k].at[1, b], minus),
            )
            for e, (src, dst, dev) in enumerate(moves):
                ring[ph, k, e] = copy_to(src, dst, rs_s.at[ph, k], rs_r.at[ph, k, min(e, 2)], dev)
            ring[ph, k, "at"] = (m, tp, tm)
    last = {}
    for k in range(4):
        name = ORDER[k][2]
        for j in range(1, 4):
            to = (pos[name] + j) % 4
            last[k, j] = copy_to(F[k].at[to], R3[k].at[j - 1], p3_s.at[k], p3_r.at[k], {name: to})
    share = [
        copy_to(GA.at[mz], GA.at[mz], gz_s.at[0], gz_r.at[0], peer("dp", j)) for j in range(1, 4)
    ]

    def exchange(buf, s, r, here, devices):
        return [copy_to(buf.at[here], buf.at[here], s, r, dev) for dev in devices], r

    plane_steps = [(i // 4, i % 4) for i in range(1, 16)]
    plane = [{"fx": (mx + i) % 4, "fy": (my + j) % 4} for i, j in plane_steps]
    cz_steps = [(i // 4, i % 4) for i in range(1, 8)]
    core_z = [{"fc": (mc + i) % 2, "dp": (mz + j) % 4} for i, j in cz_steps]

    here = mx * 4 + my
    pr0 = exchange(prc, sm_s.at[0], sm_r.at[0], mc, [partner])
    pr1 = exchange(prp, sm_s.at[1], sm_r.at[1], here, plane)
    sq0 = exchange(sqc, sm_s.at[2], sm_r.at[2], mc, [partner])
    sq1 = exchange(sqp, sm_s.at[3], sm_r.at[3], here, plane)
    nm0 = exchange(nmc, sm_s.at[4], sm_r.at[4], mc * 4 + mz, core_z)
    nm1 = exchange(nmp, sm_s.at[5], sm_r.at[5], here, plane)

    def put(copies, buf, slot, value):
        buf[slot] = value
        for copy in copies[0]:
            copy.start()

    def total(copies, buf):
        arrived(buf.at[pl.ds(0, buf.shape[0] - 1)], copies[1])
        value = buf[0]
        for j in range(1, buf.shape[0]):
            value = value + buf[j]
        return value

    load_w = pltpu.make_async_copy(w, W.at[mc, m1, m2], ld_w)
    load_w.start()
    def loaded(p, g):
        side = (oc + p) % 2
        region = T.at[side, :, pl.ds(512 * g, 512)]
        pltpu.make_async_copy(region, region, ld_t.at[p, g]).wait()

    barrier = pltpu.get_barrier_semaphore()
    others = plane + core_z
    for dev in others:
        pl.semaphore_signal(barrier, inc=1, device_id=dev, device_id_type=MESH)
    ACC[...] = jnp.zeros((512, 2048), F32)
    load_w.wait()
    load_c = pltpu.make_async_copy(cot, C, ld_c)
    load_c.start()
    for p in range(2):
        side = (oc + p) % 2
        for b in range(16):
            xy = b + side * ((b % 4) * 4 + b // 4 - b)
            pltpu.make_async_copy(
                tok.at[:, pl.ds(pl.multiple_of((2 * xy + side) * 128, 128), 128)],
                T.at[side, :, pl.ds(128 * b, 128)],
                ld_t.at[p, b // 4],
            ).start()

    w_wide = W[mc, m1, m2].astype(F32)
    lv_col = jnp.broadcast_to(lv[...], (128, 128)).T[:, 0:1]
    part_right = jnp.sum(w_wide * lv_col, axis=0, keepdims=True)
    prc[mc] = part_right
    pl.semaphore_wait(barrier, len(others))

    def spread(op):
        if op == 2:
            arrived(*landed[0, 4])
        elif op == 3:
            arrived(*landed[0, 3])
        elif op == 4:
            arrived(*landed[0, 2])
        for e in range(2):
            gather[op, e].start()
        if op != 4:
            spread_rest(op)

    def spread_rest(op):
        for e in (2, 3):
            gather[op, e].start()

    def forward(op):
        for e in range(2):
            arrived(*landed[op, e])
            gather[op, 4 + e].start()

    def cross(slot):
        for e in (2, 3, 4):
            arrived(*landed[slot + 1, e])
        across[slot].start()

    def cross_first():
        for e in (3, 4):
            arrived(*landed[4, e])
        for i in (3, 4, 5):
            across[i].start()

    def cross_last():
        arrived(*landed[4, 2])
        across[6].start()

    for copy in pr0[0]:
        copy.start()
    load_c.wait()
    give_c[0].start()
    for g in range(4):
        loaded(0, g)
        give_t[g].start()
    for copy in give_c[1:]:
        copy.start()
    put(pr1, prp, here, total(pr0, prc))
    spread(0)
    spread(1)

    def ring_go(ph, k, *events):
        for e in events:
            ring[ph, k, e].start()

    def ring_mid(ph, k):
        S, A1 = ((D, R1), (E, Q1))[ph]
        _, tp, tm = ring[ph, k, "at"]
        for d, (t, lo_, e) in enumerate(((tp, 0, 4), (tm, 2, 5))):
            arrived(A1[k].at[d], rs_r.at[ph, k, d])
            for i in range(2):
                S[k][t, lo_ + i] = (S[k][t, lo_ + i].astype(F32) + A1[k][d, i].astype(F32)).astype(BF)
            ring[ph, k, e].start()

    def mid_first():
        for k in range(2):
            @pl.when(mc == k)
            def _():
                ring_mid(1, k)

    def mid_second():
        for k in range(2):
            @pl.when(mc == 1 - k)
            def _():
                ring_mid(1, k)

    def ring_end(ph, k):
        S, A2, out = ((D, R2, E), (E, Q2, F))[ph]
        m = ring[ph, k, "at"][0]
        arrived(A2[k], rs_r.at[ph, k, 2])
        for i in range(4):
            out[k][i] = (
                S[k][m, i].astype(F32) + A2[k][0, i].astype(F32) + A2[k][1, i].astype(F32)
            ).astype(BF)

    def p1_end(k):
        ring_end(0, k)
        ring_go(1, k, 0, 1, 2, 3)

    def p2_end(k):
        ring_end(1, k)
        for j in range(1, 4):
            last[k, j].start()

    def sq_start():
        right_raw = total(pr1, prp)
        right_next = right_raw / jnp.sqrt(jnp.sum(right_raw * right_raw) + EPS)
        rn_ref[...] = right_next
        left_raw = jnp.sum(W[mc, m1, m2].astype(F32) * right_next, axis=1, keepdims=True)
        put(sq0, sqc, mc, jnp.broadcast_to(jnp.sum(left_raw * left_raw, keepdims=True), (8, 128)))

    def sq_plane():
        put(sq1, sqp, mx * 4 + my, total(sq0, sqc))

    def sq_end():
        left_sq = total(sq1, sqp)
        scal[0] = left_sq
        inv_ref[...] = 1.0 / jnp.sqrt(left_sq + EPS)

    def wait_c(turn):
        arrived(CP.at[:, quarters[turn]], ex_r.at[4 + turn])

    def wait_t(g):
        arrived(TP.at[:, pl.ds(512 * g, 512)], ex_r.at[g])
        loaded(1, g)

    wait_c(0)
    over_tokens = (((0,), (0,)), ((), ()))

    def run(events, i):
        for when, todo in events.items():
            @pl.when(i == when)
            def _():
                for f, *a in todo:
                    f(*a)

    def term(i, carry):
        turn = i // 4
        g = i % 4
        run(TERM_WAITS, i)
        q = (mz + 6 - turn) % 4
        cs = pl.ds(pl.multiple_of(q * 512, 512), 512)
        ms = pl.ds(pl.multiple_of(g * 512, 512), 512)
        r = lax.dot_general(T[mc, :, ms], C[:, cs], over_tokens, preferred_element_type=F32)
        r = r + lax.dot_general(TP[:, ms], CP[:, cs], over_tokens, preferred_element_type=F32)
        r = r.astype(BF)
        for h in range(4):
            x = g + mc * (h - g)
            y = h + mc * (g - h)
            at = ((q, x, y), (q, y, x), (x, y, q), (y, x, q))
            for k in range(4):
                for u, b, n, tile in PIECES[k]:
                    rows = slice(128 * h + b, 128 * h + b + n)
                    D[k][(*at[k], slice(u, u + n))] = r[rows, 128 * tile : 128 * tile + 128]
        run(TERM_EVENTS, i)
        return carry

    TERM_WAITS = {
        0: [(wait_t, 0)],
        1: [(wait_t, 1)],
        2: [(wait_t, 2)],
        3: [(wait_t, 3)],
        4: [(wait_c, 1)],
        8: [(wait_c, 2)],
        12: [(wait_c, 3)],
    }
    TERM_EVENTS = {
        3: [(ring_go, 0, 0, 0, 1), (ring_go, 0, 1, 0, 1)],
        5: [(sq_start,)],
        7: [(ring_go, 0, 0, 2), (ring_go, 0, 1, 2), (sq_plane,)],
        8: [(forward, 1), (forward, 0)],
        12: [(spread, 2)],
        15: [
            (ring_go, 0, 2, 0, 1, 2, 3), (ring_go, 0, 3, 0, 1, 2, 3),
            (ring_go, 0, 0, 3), (ring_go, 0, 1, 3),
        ],
    }
    lax.fori_loop(0, 16, term, 0)

    def group(slot):
        arrived(*crossed[slot])

    def norms():
        inv = inv_ref[0:1, 0:1]
        quarter = pl.ds(pl.multiple_of(mz * 512, 512), 512)
        rn = rn_ref[:, quarter]
        wq = W[mc, m1, m2, :, quarter].astype(F32)
        raw = jnp.sum(W[mc, m1, m2].astype(F32) * rn_ref[...], axis=1, keepdims=True)
        ln = raw * inv
        sums = [jnp.zeros((1, 128), F32)] * 3
        for k in range(4):
            unit = F[k][pos[ORDER[k][2]]].astype(F32)
            arrived(R3[k], p3_r.at[k])
            for j in range(3):
                unit = unit + R3[k][j].astype(F32)
            for u, b, n, tile in PIECES[k]:
                g, rows, cols = unit[u : u + n], slice(b, b + n), slice(128 * tile, 128 * tile + 128)
                GA[mz, rows, cols] = g.astype(BF)
                sums[0] = sums[0] + jnp.sum(g * g, axis=0, keepdims=True)
                sums[1] = sums[1] + jnp.sum(g * wq[rows, cols], axis=0, keepdims=True)
                sums[2] = sums[2] + jnp.sum(g * ln[rows], axis=0, keepdims=True) * rn[:, cols]
        put(nm0, nmc, mc * 4 + mz, jnp.concatenate(sums + [jnp.zeros((5, 128), F32)], axis=0))
        for copy in share:
            copy.start()

    def nm_plane():
        put(nm1, nmp, mx * 4 + my, total(nm0, nmc))

    def both(s, carry):
        run(BOTH_EVENTS, s)
        kind, i = s % 2, s // 2
        slot, other = i // 2, i % 2
        off = slot + slot // 2 - 2 * (slot // 3)
        p = (mc + other) % 2
        col = (m1 + other * (m2 - m1) + off) % 4

        @pl.when(kind == 0)
        def _():
            ms = pl.ds(pl.multiple_of(col * 512, 512), 512)
            for n in range(4):
                cs = slice(512 * n, 512 * n + 512)
                rows = W[p, col, :, :, cs].reshape(512, 512)
                ACC[:, cs] = ACC[:, cs] + jnp.dot(T[p, :, ms], rows, preferred_element_type=F32)

        @pl.when(kind == 1)
        def _():
            inv = inv_ref[0:1, 0:1]
            rows = W[p, col].reshape(512, 2048)
            r = lax.dot_general(C[...], rows, (((1,), (1,)), ((), ())), preferred_element_type=F32)
            r = (r * inv).astype(BF)
            for h in range(4):
                x = col + p * (h - col)
                y = h + p * (col - h)
                at = pl.multiple_of(((x * 4 + y) * 2 + p) * 128, 128)
                IG[:, pl.ds(at, 128)] = r[:, 128 * h : 128 * h + 128]

        return carry

    BOTH_EVENTS = {
        0: [(cross, 0)],
        1: [(sq_end,)],
        2: [(group, 0)],
        3: [(ring_mid, 0, 0), (ring_mid, 0, 1), (forward, 2)],
        4: [(ring_mid, 0, 2), (ring_mid, 0, 3), (spread, 3), (cross, 1)],
        6: [(group, 1)],
        7: [(forward, 3), (p1_end, 2), (p1_end, 3)],
        8: [(p1_end, 0), (p1_end, 1), (ring_mid, 1, 2), (ring_mid, 1, 3), (mid_first,), (cross, 2)],
        9: [(mid_second,), (spread, 4), (p2_end, 2), (p2_end, 3)],
        10: [(p2_end, 0), (p2_end, 1), (spread_rest, 4), (group, 2)],
        11: [(forward, 4)],
    }
    lax.fori_loop(0, 12, both, 0)

    def halves(s, carry):
        run(HALF_EVENTS, s)
        kind, other, late = s % 2, (s // 2) % 2, s // 4
        p = (mc + other) % 2
        a1 = (m1 + other * (m2 - m1) + 2) % 4
        base = m2 + other * (m1 - m2)
        a2 = ((base + 3 * late) % 4, (base + 1 + late) % 4)

        @pl.when(kind == 0)
        def _():
            cols = [T[p, :, pl.ds(pl.multiple_of((a1 * 4 + v) * 128, 128), 128)] for v in a2]
            toks = jnp.concatenate(cols, axis=1)
            for n in range(4):
                cs = slice(512 * n, 512 * n + 512)
                rows = jnp.concatenate([W[p, a1, v, :, cs] for v in a2], axis=0)
                ACC[:, cs] = ACC[:, cs] + jnp.dot(toks, rows, preferred_element_type=F32)

        @pl.when(kind == 1)
        def _():
            inv = inv_ref[0:1, 0:1]
            rows = jnp.concatenate([W[p, a1, v] for v in a2], axis=0)
            r = lax.dot_general(C[...], rows, (((1,), (1,)), ((), ())), preferred_element_type=F32)
            r = (r * inv).astype(BF)
            for h, v in enumerate(a2):
                x = a1 + p * (v - a1)
                y = v + p * (a1 - v)
                at = pl.multiple_of(((x * 4 + y) * 2 + p) * 128, 128)
                IG[:, pl.ds(at, 128)] = r[:, 128 * h : 128 * h + 128]

        return carry

    HALF_EVENTS = {
        0: [(norms,), (cross_first,)],
        1: [(nm_plane,)],
        2: [(group, 3), (group, 4)],
        4: [(cross_last,)],
        6: [(group, 5), (group, 6)],
    }
    lax.fori_loop(0, 8, halves, 0)

    inv = inv_ref[0:1, 0:1]
    sums = jnp.sum(total(nm1, nmp), axis=1, keepdims=True)
    grad_sq_raw, inner, crossed_term = sums[0:1], sums[1:2], sums[2:3]
    lsq = scal[0][0:1, 0:1]
    sq = lsq + EPS
    coeff = inner / sq
    rn = rn_ref[...]
    raw = jnp.sum(W[mc, m1, m2].astype(F32) * rn, axis=1, keepdims=True)
    ln = raw * inv
    ln_ref[...] = jnp.broadcast_to(ln, (128, 128)).T[0:1]
    right_unit = jnp.sum(rn * rn, keepdims=True)
    grad_sq = (
        grad_sq_raw / sq - 2.0 * coeff * crossed_term * inv + coeff * coeff * (lsq / sq) * right_unit
    )
    inv_rms = 1.0 / jnp.sqrt(grad_sq / ENTRIES + EPS)
    arrived(GA.at[pl.ds(0, 3)], gz_r.at[0])
    scale = inv * inv_rms
    column = ln * (coeff * inv_rms)
    for q in range(4):
        cs = slice(512 * q, 512 * q + 512)
        UP[:, cs] = (GA[q].astype(F32) * scale - column * rn[:, cs]).astype(BF)

    def left(size_of, sem):
        pltpu.make_async_copy(size_of, size_of, sem).wait()

    left(W.at[0, 0, pl.ds(0, 3)], ag_s.at[0])
    left(W.at[0, pl.ds(0, 3)], ag_s.at[1])
    left(W.at[0], fw_s.at[0])
    left(T, ex_s.at[0])
    for k in range(4):
        left(D[k].at[pl.ds(0, 3)], rs_s.at[0, k])
        left(E[k].at[pl.ds(0, 3)], rs_s.at[1, k])
        left(F[k].at[pl.ds(0, 3)], p3_s.at[k])
    left(GA.at[pl.ds(0, 3)], gz_s.at[0])
    for i, buf in enumerate((prc, prp, sqc, sqp, nmc, nmp)):
        left(buf.at[pl.ds(0, buf.shape[0] - 1)], sm_s.at[i])


def write_out(acc, ig, up, ln, rn, inv, lo_out, ig_out, up_out, ln_out, rn_out, lo, sems):
    copies = [
        pltpu.make_async_copy(src, dst, sems.at[i])
        for i, (src, dst) in enumerate(((ig, ig_out), (up, up_out), (ln, ln_out), (rn, rn_out)))
    ]
    for copy in copies:
        copy.start()
    for n in range(4):
        rows = pl.ds(128 * n, 128)
        lo[rows] = (acc[rows] * inv[0:1, 0:1]).astype(BF)
        copy = pltpu.make_async_copy(lo.at[rows], lo_out.at[rows], sems.at[4 + n])
        copy.start()
        copies.append(copy)
    for copy in copies:
        copy.wait()


def per_device(tokens, cotangent, weight, left_vector):
    dma = pltpu.SemaphoreType.DMA
    vm = pltpu.VMEM
    hbm = pl.BlockSpec(memory_space=pl.ANY)
    vmem = pl.BlockSpec(memory_space=pltpu.VMEM)
    outs = pl.pallas_call(
        kernel,
        out_shape=(
            vm((512, 2048), F32),
            vm((512, 4096), BF),
            vm((128, 2048), BF),
            vm((1, 128), F32),
            vm((1, 2048), F32),
            vm((8, 128), F32),
        ),
        in_specs=[hbm, hbm, hbm, vmem],
        out_specs=(vmem,) * 6,
        scratch_shapes=[
            vm((2, 4, 4, 128, 2048), BF),
            vm((2, 512, 2048), BF),
            vm((512, 2048), BF),
            vm((512, 2048), BF),
            vm((512, 2048), BF),
            *[
                vm((2, *dims, rows, 128), BF)
                for dims in ((4, 4, 4), (2, 2, 4), (2, 4, 4), (4, 4), (2, 2), (2, 4), (4,), (3,))
                for rows in ROWS
            ],
            vm((4, 128, 512), BF),
            vm((2, 1, 2048), F32),
            vm((16, 1, 2048), F32),
            vm((2, 8, 128), F32),
            vm((16, 8, 128), F32),
            vm((8, 8, 128), F32),
            vm((16, 8, 128), F32),
            vm((1, 8, 128), F32),
            dma((2,)),
            dma((5, 5)),
            dma((1,)),
            dma((7,)),
            dma((1,)),
            dma((8,)),
            dma((2, 4)),
            dma((2, 4, 3)),
            dma((4,)),
            dma((4,)),
            dma((1,)),
            dma((1,)),
            dma((6,)),
            dma((6,)),
            dma,
            dma,
            dma((2, 4)),
        ],
        compiler_params=pltpu.CompilerParams(
            collective_id=0, has_side_effects=True, vmem_limit_bytes=50 * 2**20
        ),
    )(tokens, cotangent, weight, left_vector.reshape(1, 128))
    layer_out, input_grad, update, left_next, right_next = pl.pallas_call(
        write_out,
        out_shape=(
            jax.ShapeDtypeStruct((512, 2048), BF),
            jax.ShapeDtypeStruct((512, 4096), BF),
            jax.ShapeDtypeStruct((128, 2048), BF),
            jax.ShapeDtypeStruct((1, 128), F32),
            jax.ShapeDtypeStruct((1, 2048), F32),
        ),
        in_specs=[vmem] * 6,
        out_specs=(hbm,) * 5,
        scratch_shapes=[vm((512, 2048), BF), dma((8,))],
        compiler_params=pltpu.CompilerParams(vmem_limit_bytes=6 * 2**20),
    )(*[pltpu.with_memory_space_constraint(o, pltpu.VMEM) for o in outs])
    return (layer_out, input_grad, update, left_next.reshape(128), right_next.reshape(2048))


def solution(mesh):
    torus = Mesh(mesh.devices.reshape(4, 4, 2, mesh.shape["dp"]), FSDP_DP)
    return jax.shard_map(
        per_device,
        mesh=torus,
        in_specs=(P(FSDP_DP, None), P(FSDP_DP, None), P(FSDP, None), P(FSDP)),
        out_specs=(P(FSDP_DP, None), P(FSDP_DP, None), P(FSDP, None), P(FSDP), P()),
        check_vma=False,
    )
```

```python
import jax
import jax.numpy as jnp
from jax import lax
from jax.experimental import pallas as pl
from jax.experimental.pallas import tpu as pltpu
from jax.sharding import Mesh
from jax.sharding import PartitionSpec as P

MESH = pl.DeviceIdType.MESH
BF, F32 = jnp.bfloat16, jnp.float32
EPS = 1e-06
ENTRIES = 4096 * 2048
OFFSET = (0, 1, 3, 2)
MORE = 32
ROWS = (128 + MORE, 128 - MORE)
PIECES = (
    ((0, 0, 128, 0), (128, 0, MORE, 1)),
    ((0, 0, 128, 2), (128, MORE, MORE, 1)),
    ((0, 0, 64, 3), (64, 2 * MORE, 64 - MORE, 1)),
    ((0, 64, 64, 3), (64, 64 + MORE, 64 - MORE, 1)),
)
PIECES = tuple(tuple(piece for piece in pieces if piece[2]) for pieces in PIECES)

FSDP = ("fx", "fy", "fc")
FSDP_DP = ("fx", "fy", "fc", "dp")
SIZE = {"fx": 4, "fy": 4, "fc": 2, "dp": 4}
ORDER = (("dp", "fx", "fy"), ("dp", "fy", "fx"), ("fx", "fy", "dp"), ("fy", "fx", "dp"))


def kernel(
    tok, cot, w, lv, ACC, IG, UP, ln_ref, rn_ref, inv_ref,
    W, T, TP, C, CP, Da, Db, R1a, R1b, R2a, R2b, Ea, Eb, Q1a, Q1b, Q2a, Q2b, Fa, Fb, R3a, R3b, GA,
    prc, prp, sqc, sqp, nmc, nmp, scal,
    ag_s, ag_r, fw_s, fw_r, ex_s, ex_r, rs_s, rs_r, p3_s, p3_r, gz_s, gz_r,
    sm_s, sm_r, ld_w, ld_c, ld_t,
):
    def colours(a, b):
        return [a.at[0], a.at[1], b.at[0], b.at[1]]

    D, R1, R2, E, Q1, Q2, F, R3 = (
        colours(a, b)
        for a, b in (
            (Da, Db), (R1a, R1b), (R2a, R2b), (Ea, Eb), (Q1a, Q1b), (Q2a, Q2b), (Fa, Fb), (R3a, R3b)
        )
    )
    pos = {name: lax.axis_index(name) for name in SIZE}
    mx, my, mc, mz = (pos[name] for name in ("fx", "fy", "fc", "dp"))
    oc = 1 - mc
    m1 = mx + mc * (my - mx)
    m2 = my + mc * (mx - my)

    def peer(name, step):
        return {name: (pos[name] + step) % SIZE[name]}

    def along1(step):
        return {"fx": (mx + oc * step) % 4, "fy": (my + mc * step) % 4}

    def along2(step):
        return {"fx": (mx + mc * step) % 4, "fy": (my + oc * step) % 4}

    def copy_to(src, dst, s, r, dev):
        return pltpu.make_async_remote_copy(
            src_ref=src, dst_ref=dst, send_sem=s, recv_sem=r, device_id=dev, device_id_type=MESH
        )

    def arrived(dst, sem):
        pltpu.make_async_copy(dst, dst, sem).wait()

    top, bottom, whole = pl.ds(0, 64), pl.ds(64, 64), pl.ds(0, 128)
    gather, landed = {}, {}
    for op in range(5):
        if op == 0:
            at = lambda step, rows=whole: W.at[mc, (m1 + step) % 4, m2, rows]
            dev = along1
        else:
            col = (m1 + OFFSET[op - 1]) % 4
            at = lambda step, rows=whole, col=col: W.at[mc, col, (m2 + step) % 4, rows]
            dev = along2
        moves = (
            (at(0, top), 1, 0), (at(0, bottom), 3, 1), (at(0, bottom), 1, 3), (at(0, top), 3, 4),
            (at(3, top), 1, 2), (at(1, bottom), 3, 2),
        )
        for e, (src, step, r) in enumerate(moves):
            gather[op, e] = copy_to(src, src, ag_s.at[min(op, 1)], ag_r.at[op, r], dev(step))
        for r, got in enumerate((at(3, top), at(1, bottom), at(2), at(3, bottom), at(1, top))):
            landed[op, r] = (got, ag_r.at[op, r])
    partner = peer("fc", 1)
    across, crossed = [], []
    for slot in range(3):
        mine = W.at[mc, (m1 + OFFSET[slot]) % 4]
        across.append(copy_to(mine, mine, fw_s.at[0], fw_r.at[slot], partner))
        crossed.append((W.at[oc, (m2 + OFFSET[slot]) % 4], fw_r.at[slot]))
    for step, at in enumerate(OFFSET):
        mine = W.at[mc, (m1 + 2) % 4, (m2 + at) % 4]
        across.append(copy_to(mine, mine, fw_s.at[0], fw_r.at[3 + step], partner))
        crossed.append((W.at[oc, (m2 + 2) % 4, (m1 + at) % 4], fw_r.at[3 + step]))
    quarters = [pl.ds(pl.multiple_of(((mz + 6 - turn) % 4) * 512, 512), 512) for turn in range(4)]
    give_c = [
        copy_to(C.at[:, cs], CP.at[:, cs], ex_s.at[0], ex_r.at[4 + i], partner)
        for i, cs in enumerate(quarters)
    ]
    give_t = [
        copy_to(T.at[oc, :, pl.ds(512 * g, 512)], TP.at[:, pl.ds(512 * g, 512)], ex_s.at[0], ex_r.at[g], partner)
        for g in range(4)
    ]

    ring = {}
    for ph, (S, A1, A2) in enumerate(((D, R1, R2), (E, Q1, Q2))):
        for k in range(4):
            name = ORDER[k][ph]
            m = pos[name]
            tp, tm, to = (m + 1) % 4, (m + 3) % 4, (m + 2) % 4
            plus, minus = peer(name, 1), peer(name, 3)
            a, b = pl.ds(0, 2), pl.ds(2, 2)
            moves = (
                (S[k].at[to, a], A1[k].at[0], plus),
                (S[k].at[to, b], A1[k].at[1], minus),
                (S[k].at[tp, b], A2[k].at[0, b], plus),
                (S[k].at[tm, a], A2[k].at[1, a], minus),
                (S[k].at[tp, a], A2[k].at[0, a], plus),
                (S[k].at[tm, b], A2[k].at[1, b], minus),
            )
            for e, (src, dst, dev) in enumerate(moves):
                ring[ph, k, e] = copy_to(src, dst, rs_s.at[ph, k], rs_r.at[ph, k, min(e, 2)], dev)
            ring[ph, k, "at"] = (m, tp, tm)
    last = {}
    for k in range(4):
        name = ORDER[k][2]
        for j in range(1, 4):
            to = (pos[name] + j) % 4
            last[k, j] = copy_to(F[k].at[to], R3[k].at[j - 1], p3_s.at[k], p3_r.at[k], {name: to})
    share = [
        copy_to(GA.at[mz], GA.at[mz], gz_s.at[0], gz_r.at[0], peer("dp", j)) for j in range(1, 4)
    ]

    def exchange(buf, s, r, here, devices):
        return [copy_to(buf.at[here], buf.at[here], s, r, dev) for dev in devices], r

    plane_steps = [(i // 4, i % 4) for i in range(1, 16)]
    plane = [{"fx": (mx + i) % 4, "fy": (my + j) % 4} for i, j in plane_steps]
    cz_steps = [(i // 4, i % 4) for i in range(1, 8)]
    core_z = [{"fc": (mc + i) % 2, "dp": (mz + j) % 4} for i, j in cz_steps]

    here = mx * 4 + my
    pr0 = exchange(prc, sm_s.at[0], sm_r.at[0], mc, [partner])
    pr1 = exchange(prp, sm_s.at[1], sm_r.at[1], here, plane)
    sq0 = exchange(sqc, sm_s.at[2], sm_r.at[2], mc, [partner])
    sq1 = exchange(sqp, sm_s.at[3], sm_r.at[3], here, plane)
    nm0 = exchange(nmc, sm_s.at[4], sm_r.at[4], mc * 4 + mz, core_z)
    nm1 = exchange(nmp, sm_s.at[5], sm_r.at[5], here, plane)

    def put(copies, buf, slot, value):
        buf[slot] = value
        for copy in copies[0]:
            copy.start()

    def total(copies, buf):
        arrived(buf.at[pl.ds(0, buf.shape[0] - 1)], copies[1])
        value = buf[0]
        for j in range(1, buf.shape[0]):
            value = value + buf[j]
        return value

    load_w = pltpu.make_async_copy(w, W.at[mc, m1, m2], ld_w)
    load_w.start()
    def loaded(p, g):
        side = (oc + p) % 2
        region = T.at[side, :, pl.ds(512 * g, 512)]
        pltpu.make_async_copy(region, region, ld_t.at[p, g]).wait()

    barrier = pltpu.get_barrier_semaphore()
    others = plane + core_z
    for dev in others:
        pl.semaphore_signal(barrier, inc=1, device_id=dev, device_id_type=MESH)
    ACC[...] = jnp.zeros((512, 2048), F32)
    load_w.wait()
    load_c = pltpu.make_async_copy(cot, C, ld_c)
    load_c.start()
    for p in range(2):
        side = (oc + p) % 2
        for b in range(16):
            xy = b + side * ((b % 4) * 4 + b // 4 - b)
            pltpu.make_async_copy(
                tok.at[:, pl.ds(pl.multiple_of((2 * xy + side) * 128, 128), 128)],
                T.at[side, :, pl.ds(128 * b, 128)],
                ld_t.at[p, b // 4],
            ).start()

    w_wide = W[mc, m1, m2].astype(F32)
    lv_col = jnp.broadcast_to(lv[...], (128, 128)).T[:, 0:1]
    part_right = jnp.sum(w_wide * lv_col, axis=0, keepdims=True)
    prc[mc] = part_right
    pl.semaphore_wait(barrier, len(others))

    def spread(op):
        if op == 2:
            arrived(*landed[0, 4])
        elif op == 3:
            arrived(*landed[0, 3])
        elif op == 4:
            arrived(*landed[0, 2])
        for e in range(2):
            gather[op, e].start()
        if op < 3:
            spread_rest(op)

    def spread_rest(op):
        for e in (2, 3):
            gather[op, e].start()

    def forward(op):
        for e in range(2):
            arrived(*landed[op, e])
            gather[op, 4 + e].start()

    def cross(slot):
        for e in (2, 3, 4):
            arrived(*landed[slot + 1, e])
        across[slot].start()

    def cross_first():
        for e in (3, 4):
            arrived(*landed[4, e])
        for i in (3, 4, 5):
            across[i].start()

    def cross_last():
        arrived(*landed[4, 2])
        across[6].start()

    for copy in pr0[0]:
        copy.start()
    load_c.wait()
    give_c[0].start()
    for g in range(4):
        loaded(0, g)
        give_t[g].start()
    for copy in give_c[1:]:
        copy.start()
    put(pr1, prp, here, total(pr0, prc))
    spread(0)
    spread(1)

    def ring_go(ph, k, *events):
        for e in events:
            ring[ph, k, e].start()

    def ring_mid(ph, k):
        S, A1 = ((D, R1), (E, Q1))[ph]
        _, tp, tm = ring[ph, k, "at"]
        for d, (t, lo_, e) in enumerate(((tp, 0, 4), (tm, 2, 5))):
            arrived(A1[k].at[d], rs_r.at[ph, k, d])
            for i in range(2):
                S[k][t, lo_ + i] = (S[k][t, lo_ + i].astype(F32) + A1[k][d, i].astype(F32)).astype(BF)
            ring[ph, k, e].start()

    def mid_first(ph, k0):
        for k in range(2):
            @pl.when(mc == k)
            def _():
                ring_mid(ph, k0 + k)

    def mid_second(ph, k0):
        for k in range(2):
            @pl.when(mc == 1 - k)
            def _():
                ring_mid(ph, k0 + k)

    def ring_end(ph, k):
        S, A2, out = ((D, R2, E), (E, Q2, F))[ph]
        m = ring[ph, k, "at"][0]
        arrived(A2[k], rs_r.at[ph, k, 2])
        for i in range(4):
            out[k][i] = (
                S[k][m, i].astype(F32) + A2[k][0, i].astype(F32) + A2[k][1, i].astype(F32)
            ).astype(BF)

    def p1_end(k):
        ring_end(0, k)
        ring_go(1, k, 0, 1, 2, 3)

    def p2_end(k):
        ring_end(1, k)
        for j in range(1, 4):
            last[k, j].start()

    def sq_start():
        right_raw = total(pr1, prp)
        right_next = right_raw / jnp.sqrt(jnp.sum(right_raw * right_raw) + EPS)
        rn_ref[...] = right_next
        left_raw = jnp.sum(W[mc, m1, m2].astype(F32) * right_next, axis=1, keepdims=True)
        put(sq0, sqc, mc, jnp.broadcast_to(jnp.sum(left_raw * left_raw, keepdims=True), (8, 128)))

    def sq_plane():
        put(sq1, sqp, mx * 4 + my, total(sq0, sqc))

    def sq_end():
        left_sq = total(sq1, sqp)
        scal[0] = left_sq
        inv_ref[...] = 1.0 / jnp.sqrt(left_sq + EPS)

    def wait_c(turn):
        arrived(CP.at[:, quarters[turn]], ex_r.at[4 + turn])

    def wait_t(g):
        arrived(TP.at[:, pl.ds(512 * g, 512)], ex_r.at[g])
        loaded(1, g)

    wait_c(0)
    over_tokens = (((0,), (0,)), ((), ()))

    def run(events, i):
        for when, todo in events.items():
            @pl.when(i == when)
            def _():
                for f, *a in todo:
                    f(*a)

    def term(i, carry):
        turn = i // 4
        g = i % 4
        run(TERM_WAITS, i)
        q = (mz + 6 - turn) % 4
        cs = pl.ds(pl.multiple_of(q * 512, 512), 512)
        ms = pl.ds(pl.multiple_of(g * 512, 512), 512)
        r = lax.dot_general(T[mc, :, ms], C[:, cs], over_tokens, preferred_element_type=F32)
        r = r + lax.dot_general(TP[:, ms], CP[:, cs], over_tokens, preferred_element_type=F32)
        r = r.astype(BF)
        for h in range(4):
            x = g + mc * (h - g)
            y = h + mc * (g - h)
            at = ((q, x, y), (q, y, x), (x, y, q), (y, x, q))
            for k in range(4):
                for u, b, n, tile in PIECES[k]:
                    rows = slice(128 * h + b, 128 * h + b + n)
                    D[k][(*at[k], slice(u, u + n))] = r[rows, 128 * tile : 128 * tile + 128]
        run(TERM_EVENTS, i)
        return carry

    TERM_WAITS = {
        0: [(wait_t, 0)],
        1: [(wait_t, 1)],
        2: [(wait_t, 2)],
        3: [(wait_t, 3)],
        4: [(wait_c, 1)],
        8: [(wait_c, 2)],
        12: [(wait_c, 3)],
    }
    TERM_EVENTS = {
        3: [(ring_go, 0, 0, 0, 1), (ring_go, 0, 1, 0, 1)],
        5: [(sq_start,)],
        7: [(ring_go, 0, 0, 2), (ring_go, 0, 1, 2), (sq_plane,)],
        8: [(forward, 1), (forward, 0)],
        11: [(spread, 2)],
        15: [
            (ring_go, 0, 2, 0, 1, 2, 3), (ring_go, 0, 3, 0, 1, 2, 3),
            (ring_go, 0, 0, 3), (ring_go, 0, 1, 3),
        ],
    }
    lax.fori_loop(0, 16, term, 0)

    def group(slot):
        arrived(*crossed[slot])

    def norms():
        inv = inv_ref[0:1, 0:1]
        quarter = pl.ds(pl.multiple_of(mz * 512, 512), 512)
        rn = rn_ref[:, quarter]
        wq = W[mc, m1, m2, :, quarter].astype(F32)
        raw = jnp.sum(W[mc, m1, m2].astype(F32) * rn_ref[...], axis=1, keepdims=True)
        ln = raw * inv
        sums = [jnp.zeros((1, 128), F32)] * 3
        for k in range(4):
            unit = F[k][pos[ORDER[k][2]]].astype(F32)
            arrived(R3[k], p3_r.at[k])
            for j in range(3):
                unit = unit + R3[k][j].astype(F32)
            for u, b, n, tile in PIECES[k]:
                g, rows, cols = unit[u : u + n], slice(b, b + n), slice(128 * tile, 128 * tile + 128)
                GA[mz, rows, cols] = g.astype(BF)
                sums[0] = sums[0] + jnp.sum(g * g, axis=0, keepdims=True)
                sums[1] = sums[1] + jnp.sum(g * wq[rows, cols], axis=0, keepdims=True)
                sums[2] = sums[2] + jnp.sum(g * ln[rows], axis=0, keepdims=True) * rn[:, cols]
        put(nm0, nmc, mc * 4 + mz, jnp.concatenate(sums + [jnp.zeros((5, 128), F32)], axis=0))
        for copy in share:
            copy.start()

    def nm_plane():
        put(nm1, nmp, mx * 4 + my, total(nm0, nmc))

    def both(s, carry):
        run(BOTH_EVENTS, s)
        kind, i = s % 2, s // 2
        slot, other = i // 2, i % 2
        off = slot + slot // 2 - 2 * (slot // 3)
        p = (mc + other) % 2
        col = (m1 + other * (m2 - m1) + off) % 4

        @pl.when(kind == 0)
        def _():
            ms = pl.ds(pl.multiple_of(col * 512, 512), 512)
            for n in range(4):
                cs = slice(512 * n, 512 * n + 512)
                rows = W[p, col, :, :, cs].reshape(512, 512)
                ACC[:, cs] = ACC[:, cs] + jnp.dot(T[p, :, ms], rows, preferred_element_type=F32)

        @pl.when(kind == 1)
        def _():
            inv = inv_ref[0:1, 0:1]
            rows = W[p, col].reshape(512, 2048)
            r = lax.dot_general(C[...], rows, (((1,), (1,)), ((), ())), preferred_element_type=F32)
            r = (r * inv).astype(BF)
            for h in range(4):
                x = col + p * (h - col)
                y = h + p * (col - h)
                at = pl.multiple_of(((x * 4 + y) * 2 + p) * 128, 128)
                IG[:, pl.ds(at, 128)] = r[:, 128 * h : 128 * h + 128]

        return carry

    BOTH_EVENTS = {
        0: [(cross, 0)],
        1: [(sq_end,)],
        2: [(group, 0)],
        3: [(ring_mid, 0, 0), (ring_mid, 0, 1), (forward, 2)],
        4: [(mid_first, 0, 2), (spread, 3), (mid_second, 0, 2), (spread_rest, 3), (cross, 1)],
        6: [(group, 1)],
        7: [(forward, 3), (p1_end, 2), (p1_end, 3)],
        8: [(p1_end, 0), (p1_end, 1), (ring_mid, 1, 2), (ring_mid, 1, 3), (mid_first, 1, 0), (cross, 2)],
        9: [(mid_second, 1, 0), (spread, 4), (p2_end, 2), (p2_end, 3)],
        10: [(p2_end, 0), (p2_end, 1), (spread_rest, 4), (group, 2)],
        11: [(forward, 4)],
    }
    lax.fori_loop(0, 12, both, 0)

    def halves(s, carry):
        run(HALF_EVENTS, s)
        kind, other, late = s % 2, (s // 2) % 2, s // 4
        p = (mc + other) % 2
        a1 = (m1 + other * (m2 - m1) + 2) % 4
        base = m2 + other * (m1 - m2)
        a2 = ((base + 3 * late) % 4, (base + 1 + late) % 4)

        @pl.when(kind == 0)
        def _():
            cols = [T[p, :, pl.ds(pl.multiple_of((a1 * 4 + v) * 128, 128), 128)] for v in a2]
            toks = jnp.concatenate(cols, axis=1)
            for n in range(4):
                cs = slice(512 * n, 512 * n + 512)
                rows = jnp.concatenate([W[p, a1, v, :, cs] for v in a2], axis=0)
                ACC[:, cs] = ACC[:, cs] + jnp.dot(toks, rows, preferred_element_type=F32)

        @pl.when(kind == 1)
        def _():
            inv = inv_ref[0:1, 0:1]
            rows = jnp.concatenate([W[p, a1, v] for v in a2], axis=0)
            r = lax.dot_general(C[...], rows, (((1,), (1,)), ((), ())), preferred_element_type=F32)
            r = (r * inv).astype(BF)
            for h, v in enumerate(a2):
                x = a1 + p * (v - a1)
                y = v + p * (a1 - v)
                at = pl.multiple_of(((x * 4 + y) * 2 + p) * 128, 128)
                IG[:, pl.ds(at, 128)] = r[:, 128 * h : 128 * h + 128]

        return carry

    HALF_EVENTS = {
        0: [(norms,), (cross_first,)],
        2: [(nm_plane,), (group, 3), (group, 4)],
        4: [(cross_last,)],
        6: [(group, 5), (group, 6)],
    }
    lax.fori_loop(0, 8, halves, 0)

    inv = inv_ref[0:1, 0:1]
    sums = jnp.sum(total(nm1, nmp), axis=1, keepdims=True)
    grad_sq_raw, inner, crossed_term = sums[0:1], sums[1:2], sums[2:3]
    lsq = scal[0][0:1, 0:1]
    sq = lsq + EPS
    coeff = inner / sq
    rn = rn_ref[...]
    raw = jnp.sum(W[mc, m1, m2].astype(F32) * rn, axis=1, keepdims=True)
    ln = raw * inv
    ln_ref[...] = jnp.broadcast_to(ln, (128, 128)).T[0:1]
    right_unit = jnp.sum(rn * rn, keepdims=True)
    grad_sq = (
        grad_sq_raw / sq - 2.0 * coeff * crossed_term * inv + coeff * coeff * (lsq / sq) * right_unit
    )
    inv_rms = 1.0 / jnp.sqrt(grad_sq / ENTRIES + EPS)
    arrived(GA.at[pl.ds(0, 3)], gz_r.at[0])
    scale = inv * inv_rms
    column = ln * (coeff * inv_rms)
    for q in range(4):
        cs = slice(512 * q, 512 * q + 512)
        UP[:, cs] = (GA[q].astype(F32) * scale - column * rn[:, cs]).astype(BF)

    def left(size_of, sem):
        pltpu.make_async_copy(size_of, size_of, sem).wait()

    left(W.at[0, 0, pl.ds(0, 3)], ag_s.at[0])
    left(W.at[0, pl.ds(0, 3)], ag_s.at[1])
    left(W.at[0], fw_s.at[0])
    left(T, ex_s.at[0])
    for k in range(4):
        left(D[k].at[pl.ds(0, 3)], rs_s.at[0, k])
        left(E[k].at[pl.ds(0, 3)], rs_s.at[1, k])
        left(F[k].at[pl.ds(0, 3)], p3_s.at[k])
    left(GA.at[pl.ds(0, 3)], gz_s.at[0])
    for i, buf in enumerate((prc, prp, sqc, sqp, nmc, nmp)):
        left(buf.at[pl.ds(0, buf.shape[0] - 1)], sm_s.at[i])


def write_out(acc, ig, up, ln, rn, inv, lo_out, ig_out, up_out, ln_out, rn_out, lo, sems):
    copies = [
        pltpu.make_async_copy(src, dst, sems.at[i])
        for i, (src, dst) in enumerate(((ig, ig_out), (up, up_out), (ln, ln_out), (rn, rn_out)))
    ]
    for copy in copies:
        copy.start()
    for n in range(4):
        rows = pl.ds(128 * n, 128)
        lo[rows] = (acc[rows] * inv[0:1, 0:1]).astype(BF)
        copy = pltpu.make_async_copy(lo.at[rows], lo_out.at[rows], sems.at[4 + n])
        copy.start()
        copies.append(copy)
    for copy in copies:
        copy.wait()


def per_device(tokens, cotangent, weight, left_vector):
    dma = pltpu.SemaphoreType.DMA
    vm = pltpu.VMEM
    hbm = pl.BlockSpec(memory_space=pl.ANY)
    vmem = pl.BlockSpec(memory_space=pltpu.VMEM)
    outs = pl.pallas_call(
        kernel,
        out_shape=(
            vm((512, 2048), F32),
            vm((512, 4096), BF),
            vm((128, 2048), BF),
            vm((1, 128), F32),
            vm((1, 2048), F32),
            vm((8, 128), F32),
        ),
        in_specs=[hbm, hbm, hbm, vmem],
        out_specs=(vmem,) * 6,
        scratch_shapes=[
            vm((2, 4, 4, 128, 2048), BF),
            vm((2, 512, 2048), BF),
            vm((512, 2048), BF),
            vm((512, 2048), BF),
            vm((512, 2048), BF),
            *[
                vm((2, *dims, rows, 128), BF)
                for dims in ((4, 4, 4), (2, 2, 4), (2, 4, 4), (4, 4), (2, 2), (2, 4), (4,), (3,))
                for rows in ROWS
            ],
            vm((4, 128, 512), BF),
            vm((2, 1, 2048), F32),
            vm((16, 1, 2048), F32),
            vm((2, 8, 128), F32),
            vm((16, 8, 128), F32),
            vm((8, 8, 128), F32),
            vm((16, 8, 128), F32),
            vm((1, 8, 128), F32),
            dma((2,)),
            dma((5, 5)),
            dma((1,)),
            dma((7,)),
            dma((1,)),
            dma((8,)),
            dma((2, 4)),
            dma((2, 4, 3)),
            dma((4,)),
            dma((4,)),
            dma((1,)),
            dma((1,)),
            dma((6,)),
            dma((6,)),
            dma,
            dma,
            dma((2, 4)),
        ],
        compiler_params=pltpu.CompilerParams(
            collective_id=0, has_side_effects=True, vmem_limit_bytes=50 * 2**20
        ),
    )(tokens, cotangent, weight, left_vector.reshape(1, 128))
    layer_out, input_grad, update, left_next, right_next = pl.pallas_call(
        write_out,
        out_shape=(
            jax.ShapeDtypeStruct((512, 2048), BF),
            jax.ShapeDtypeStruct((512, 4096), BF),
            jax.ShapeDtypeStruct((128, 2048), BF),
            jax.ShapeDtypeStruct((1, 128), F32),
            jax.ShapeDtypeStruct((1, 2048), F32),
        ),
        in_specs=[vmem] * 6,
        out_specs=(hbm,) * 5,
        scratch_shapes=[vm((512, 2048), BF), dma((8,))],
        compiler_params=pltpu.CompilerParams(vmem_limit_bytes=6 * 2**20),
    )(*[pltpu.with_memory_space_constraint(o, pltpu.VMEM) for o in outs])
    return (layer_out, input_grad, update, left_next.reshape(128), right_next.reshape(2048))


def solution(mesh):
    torus = Mesh(mesh.devices.reshape(4, 4, 2, mesh.shape["dp"]), FSDP_DP)
    return jax.shard_map(
        per_device,
        mesh=torus,
        in_specs=(P(FSDP_DP, None), P(FSDP_DP, None), P(FSDP, None), P(FSDP)),
        out_specs=(P(FSDP_DP, None), P(FSDP_DP, None), P(FSDP, None), P(FSDP), P()),
        check_vma=False,
    )
```
